256 devices in a mesh: section: 8 (over y_hi, x), sta: 32 (over z, y_lo, core).
Axes of the slice: x: 4, y: 4 (y_hi: 2, y_lo: 2; y = y_hi * 2 + y_lo), z: 8, core: 2. Of those that a mesh axis runs over, the one named last changes fastest.
Arguments:
- waveforms: bfloat16 [8, 256, 8, 4096], P('section', 'sta'), may hold values from -6 to 6
- segment_mask: int32 [8, 256, 8], P('section', 'sta'), may hold values 0 or 1
- pair_blocks: int32 [32, 4], P('sta'), may hold values from 0 to 31, as said below
- window_decay: float32 [8], P('section'), may hold values from 0.5 to 1
Outputs:
- stacked: bfloat16 [8, 256, 32, 384], P('section', 'sta')
The draws below stay inside these ranges and needn't reach their ends.
Inputs may be any that keep to these rules, and one draw needn't show every extreme that they name: `pair_blocks`: entry k of row b names a block of 8 stations other than b; entries of a row may repeat.
All inputs are finite; a program needn't handle non-finite values. No bound on the sum of `segment_mask` on one device may be relied on, other than what follows from the above.
Results may differ from the reference program's by a relative error of at most 0.008.
Values may be sent and summed in bfloat16 or wider, within the bound.
No kernel may reach another device: no remote copies, remote signals or barrier semaphores. Data moves between devices by JAX's collectives and lax.ppermute only.
A program may use at most 64 MiB of HBM per device.

```python
import math
import jax
import jax.numpy as jnp
from jax import lax

RADIX = 64
NF = 1024
LAGS = 384
SMOOTH_HALF = 32
PB = 4
LS = 8
SEGS = 8
NSAMP = 4096
BLOCKS = 32
STATIONS = 256
PARTNERS = 32
WINDOWS = 8


def draw_pair_blocks(key, part):
    offsets = jax.random.randint(key, (BLOCKS, PB), 1, BLOCKS)
    block_ids = jnp.arange(BLOCKS, dtype=jnp.int32)[:, None]
    return ((block_ids + offsets) % BLOCKS).astype(jnp.int32)


def plant(drawn, rng, low, high):
    spot = [jax.random.randint(jax.random.fold_in(rng, axis), (), 0, length) for axis, length in enumerate(drawn.shape)]
    widest = drawn.shape.index(max(drawn.shape))
    beside = spot[:widest] + [(spot[widest] + 1) % drawn.shape[widest]] + spot[widest + 1:]
    return drawn.at[tuple(spot)].set(low).at[tuple(beside)].set(high)


def block_scale(own_key, shape, shards, least, top_value):
    level = 1.0
    for dim, blocks in shards:
        heights = jax.random.uniform(jax.random.fold_in(jax.random.fold_in(own_key, 6), dim), (blocks,), jnp.float32, least / len(shards), top_value / len(shards))
        level = level * jnp.repeat(jnp.exp(heights), shape[dim] // blocks).reshape((-1,) + (1,) * (len(shape) - 1 - dim))
    return level


def centred(rng, extent, deviation, reach, shards=(), held_as=jnp.bfloat16):
    drawn = deviation * jax.random.normal(rng, extent, jnp.float32)
    if shards:
        drawn = drawn * block_scale(rng, extent, shards, -0.22, 0.18)
    return jnp.clip(drawn, -reach, reach).astype(held_as)


def setup_inputs(seed: int = 0) -> dict:
    streams_of = jax.random.split(jax.random.key(seed), 5)
    return {
        "waveforms": centred(streams_of[0], (WINDOWS, STATIONS, SEGS, NSAMP), 1.0, 6.0, ((0, 8), (1, 32))),
        "segment_mask": plant((jax.random.randint(streams_of[1], (WINDOWS, STATIONS, SEGS), 0, 2) < 1).astype(jnp.int32), jax.random.fold_in(streams_of[1], 1), 0, 1),
        "pair_blocks": draw_pair_blocks(jax.random.fold_in(streams_of[4], 71), 0),
        "window_decay": jnp.clip(0.5 + 0.5 * jax.random.uniform(streams_of[3], (WINDOWS,), jnp.float32) ** block_scale(streams_of[3], (WINDOWS,), ((0, 8),), -0.2, 0.2), 0.5, 1.0),
    }


epsilon = 1e-05

def band_spectrum(waves):
    spectrum = jnp.fft.rfft(waves.astype(jnp.float32), axis=-1)
    lowest = 2 * RADIX
    spectrum = spectrum[..., lowest:lowest + NF] / RADIX
    return (jnp.real(spectrum), jnp.imag(spectrum))

def whiten(spec_real, spec_imag):
    amplitude = jnp.sqrt(spec_real * spec_real + spec_imag * spec_imag)
    widths = [(0, 0)] * (amplitude.ndim - 1) + [(SMOOTH_HALF, SMOOTH_HALF)]
    padded = jnp.pad(amplitude, widths)
    smooth = jnp.zeros_like(amplitude)
    for offset in range(2 * SMOOTH_HALF + 1):
        smooth = smooth + padded[..., offset:offset + NF]
    smooth = smooth / (2 * SMOOTH_HALF + 1)
    white_real = (spec_real / (smooth + epsilon)).astype(jnp.bfloat16)
    white_imag = (spec_imag / (smooth + epsilon)).astype(jnp.bfloat16)
    return (white_real, white_imag)

def lag_table():
    freq_bins = 2 * RADIX + jnp.arange(NF, dtype=jnp.int32)
    lag_shift = jnp.arange(LAGS, dtype=jnp.int32) + RADIX * RADIX - LAGS // 2
    phase = (freq_bins[:, None] * lag_shift[None, :] % (RADIX * RADIX)).astype(jnp.float32) * (2.0 * jnp.pi / (RADIX * RADIX))
    table = jnp.concatenate([jnp.cos(phase), -jnp.sin(phase)], axis=0) / math.sqrt(NF)
    return table.astype(jnp.bfloat16)

def correlate(local_real, local_imag, local_marks, part_real, part_imag, part_marks, table):
    mine_real = local_real.astype(jnp.float32) * local_marks[:, :, None]
    mine_imag = local_imag.astype(jnp.float32) * local_marks[:, :, None]
    other_real = part_real.astype(jnp.float32) * part_marks[:, :, None]
    other_imag = part_imag.astype(jnp.float32) * part_marks[:, :, None]
    cross_real = jnp.einsum('isf,jsf->ijf', mine_real, other_real) + jnp.einsum('isf,jsf->ijf', mine_imag, other_imag)
    cross_imag = jnp.einsum('isf,jsf->ijf', mine_real, other_imag) - jnp.einsum('isf,jsf->ijf', mine_imag, other_real)
    count = jnp.einsum('is,js->ij', local_marks, part_marks)
    divisor = jnp.maximum(count, 1.0)[:, :, None]
    cross = (jnp.concatenate([cross_real, cross_imag], axis=-1) / divisor).astype(jnp.bfloat16)
    lagged = jnp.dot(cross.reshape(-1, 2 * NF), table, preferred_element_type=jnp.float32)
    return lagged.reshape(local_real.shape[0], part_real.shape[0], LAGS)

def reference(waveforms, segment_mask, pair_blocks, window_decay):
    table = lag_table()

    def one_window(state, inputs):
        waves, marks, decay = inputs
        spec_real, spec_imag = band_spectrum(waves)
        white_real, white_imag = whiten(spec_real, spec_imag)
        marks = marks.astype(jnp.float32)
        blocks_real = white_real.reshape(BLOCKS, LS, SEGS, NF)
        blocks_imag = white_imag.reshape(BLOCKS, LS, SEGS, NF)
        blocks_marks = marks.reshape(BLOCKS, LS, SEGS)

        def per_block(items):
            local_real, local_imag, local_marks, chosen = items
            part_real = jnp.take(blocks_real, chosen, axis=0).reshape(PB * LS, SEGS, NF)
            part_imag = jnp.take(blocks_imag, chosen, axis=0).reshape(PB * LS, SEGS, NF)
            part_marks = jnp.take(blocks_marks, chosen, axis=0).reshape(PB * LS, SEGS)
            return correlate(local_real, local_imag, local_marks, part_real, part_imag, part_marks, table)
        lagged = lax.map(per_block, (blocks_real, blocks_imag, blocks_marks, pair_blocks))
        lagged = lagged.reshape(STATIONS, PARTNERS, LAGS)
        state = decay * state + lagged
        return (state, state.astype(jnp.bfloat16))
    initial = jnp.zeros((STATIONS, PARTNERS, LAGS), jnp.float32)
    final_state, stacked = lax.scan(one_window, initial, (waveforms, segment_mask, window_decay))
    return stacked
```

```python
import functools
import math

import jax
import jax.numpy as jnp
import numpy as np
from jax import lax
from jax.experimental import pallas as pl
from jax.experimental.pallas import tpu as pltpu
from jax.sharding import PartitionSpec as P

NF = 1024
LAGS = 384
NSAMP = 4096
LS = 8
SEGS = 8
PB = 4
EPSILON = 1e-05
CHUNKS = (4, 4)
INTERPRET = False


def twiddles():
    k = np.arange(32)[:, None]
    b = np.arange(128)[None, :]
    angle = 2.0 * np.pi * (k * b) / NSAMP
    return np.stack([np.cos(angle), np.sin(angle)]).astype(np.float32)


def second_dft():
    b = np.arange(128)[:, None]
    m = np.arange(4, 36)[None, :]
    angle = 2.0 * np.pi * ((b * m) % 128) / 128
    cos, sin = np.cos(angle) / 64, np.sin(angle) / 64
    full = np.zeros((4, 256, 256))
    for klo in range(4):
        at = 32 * klo
        full[klo, :128, at : at + 32] = cos
        full[klo, 128:, at : at + 32] = sin
        full[klo, :128, 128 + at : 160 + at] = -sin
        full[klo, 128:, 128 + at : 160 + at] = cos
    high = full.astype(jnp.bfloat16)
    low = (full - high.astype(np.float64)).astype(jnp.bfloat16)
    return np.stack([high, low])


def lag_table():
    freq = 128 + np.arange(NF)
    shift = np.arange(LAGS) + NSAMP - LAGS // 2
    phase = (freq[:, None] * shift[None, :] % NSAMP).astype(np.float32)
    phase = phase * np.float32(2.0 * np.pi / NSAMP)
    cos = np.cos(phase) / np.float32(math.sqrt(NF))
    sin = -np.sin(phase) / np.float32(math.sqrt(NF))
    lane = np.arange(128)
    rows = []
    for c in range(8):
        f = 8 * (lane // 32) + c + 32 * (lane % 32)
        rows += [cos[f], sin[f]]
    return np.concatenate(rows).astype(jnp.bfloat16)


def add(a, b):
    return b if a is None else a if b is None else a + b


def sub(a, b):
    if b is None:
        return a
    return -b if a is None else a - b


def real_fft(xs):
    n = len(xs)
    if n == 1:
        return [(xs[0], None)]
    if n == 2:
        return [(xs[0] + xs[1], None), (xs[0] - xs[1], None)]
    even, odd = real_fft(xs[0::2]), real_fft(xs[1::2])
    out = [None] * (n // 2 + 1)
    for k in range(n // 4 + 1):
        (er, ei), (orr, oi) = even[k], odd[k]
        if k == 0:
            tr, ti = orr, oi
        elif 4 * k == n:
            tr, ti = oi, None if orr is None else -orr
        else:
            c, s = math.cos(2 * math.pi * k / n), math.sin(2 * math.pi * k / n)
            if oi is None:
                tr, ti = orr * c, orr * (-s)
            else:
                tr, ti = orr * c + oi * s, oi * c - orr * s
        out[k] = (add(er, tr), add(ei, ti))
        out[n // 2 - k] = (sub(er, tr), sub(ti, ei))
    return out


def spectrum_kernel(place_ref, wave_ref, mask_ref, turn_ref, dft_ref, *refs):
    outs, (mid, white) = refs[:-2], refs[-2:]
    for i in range(LS):
        xs = [wave_ref[i, :, 128 * a : 128 * (a + 1)].astype(jnp.float32) for a in range(32)]
        half = real_fft(xs)
        for k in range(32):
            re, im = half[k] if k <= 16 else half[32 - k]
            if k > 16 and im is not None:
                im = -im
            if k:
                cos, sin = turn_ref[0, k : k + 1, :], turn_ref[1, k : k + 1, :]
                if im is None:
                    re, im = re * cos, -(re * sin)
                else:
                    re, im = re * cos + im * sin, im * cos - re * sin
            klo, c = divmod(k, 8)
            row = c * 64 + i * 8
            mid[klo, row : row + 8, :128] = re
            mid[klo, row : row + 8, 128:] = jnp.zeros_like(re) if im is None else im
    acc = jnp.zeros((512, 256), jnp.float32)
    for klo in range(4):
        value = mid[klo]
        high = value.astype(jnp.bfloat16)
        low = (value - high.astype(jnp.float32)).astype(jnp.bfloat16)
        wh, wl = dft_ref[0, klo], dft_ref[1, klo]
        dot = functools.partial(jnp.dot, preferred_element_type=jnp.float32)
        acc = acc + (dot(high, wh) + (dot(low, wh) + dot(high, wl)))
    re, im = acc[:, :128], acc[:, 128:]
    amp = jnp.sqrt(re * re + im * im)
    amps = [amp[64 * c : 64 * (c + 1)] for c in range(8)]
    before, after = [amps[0]], [amps[7]]
    for c in range(1, 8):
        before.append(before[-1] + amps[c])
        after.append(after[-1] + amps[7 - c])
    after = after[::-1]
    total = before[7]
    lane = lax.broadcasted_iota(jnp.int32, (64, 128), 1)
    klo = lane // 32
    m = lane % 32
    turned = [pltpu.roll(total, 32 * d, 1) for d in (1, 2, 3)]
    zero = jnp.zeros_like(total)
    all_klo = total + turned[0] + turned[1] + turned[2]
    lower = upper = zero
    for d in (1, 2, 3):
        lower = lower + jnp.where(klo >= d, turned[d - 1], zero)
        upper = upper + jnp.where(klo + d <= 3, turned[3 - d], zero)
    for c in range(8):
        left = pltpu.roll(after[c] + upper, 1, 1)
        right = pltpu.roll(before[c] + lower, 127, 1)
        smooth = all_klo + jnp.where(m >= 1, left, zero) + jnp.where(m <= 30, right, zero)
        scale = mask_ref[...] / (smooth * (1.0 / 65) + EPSILON)
        rows = slice(64 * c, 64 * (c + 1))
        white[0, rows, :] = re[rows] * scale
        white[1, rows, :] = im[rows] * scale
    place = place_ref[0]
    count = len(CHUNKS)
    for r in range(4):
        for e in range(2):
            seg = 2 * (place ^ r) + e
            c = 0
            for h in range(count):
                out = outs[r * count + h]
                for local in range(CHUNKS[h]):
                    at = pl.ds(64 * c + seg, 8, stride=8)
                    tile = jnp.concatenate([white[0, at, :], white[1, at, :]], axis=0)
                    out[2 * local + e] = tile.astype(jnp.bfloat16)
                    c += 1
        seg = 2 * (place ^ r)
        tile = [mask_ref[pl.ds(seg + e, 8, stride=8), :] for e in range(2)]
        outs[r * count][2 * CHUNKS[0]] = jnp.concatenate(tile, axis=0).astype(jnp.bfloat16)


def tiles_of(h):
    return 2 * CHUNKS[h] + (h == 0)


def spectrum(waves, mask, place):
    shapes = [
        jax.ShapeDtypeStruct((tiles_of(h), 16, 128), jnp.bfloat16)
        for _ in range(4)
        for h in range(len(CHUNKS))
    ]
    vmem = pl.BlockSpec(memory_space=pltpu.VMEM)
    return pl.pallas_call(
        spectrum_kernel,
        out_shape=shapes,
        in_specs=[pl.BlockSpec(memory_space=pltpu.SMEM)] + [vmem] * 4,
        out_specs=[vmem] * len(shapes),
        scratch_shapes=[
            pltpu.VMEM((4, 512, 256), jnp.float32),
            pltpu.VMEM((2, 512, 128), jnp.float32),
        ],
        interpret=INTERPRET,
        name="spectrum",
    )(place, waves, mask, jnp.asarray(twiddles()), jnp.asarray(second_dft()))


def select_kernel(place_ref, *refs):
    pairs, planes, outs, held = refs[:4], refs[4:12], refs[12:16], refs[16]
    for dz in range(8):
        held[dz] = planes[dz][...]
    z, mate = place_ref[1], place_ref[0]
    for r in range(4):
        for k in range(PB):
            p = pairs[r][0, k]
            dz = ((p // 4) - z + 8) % 8
            outs[r][k] = held[dz, (p % 4) ^ mate]


def select(place, pairs, planes):
    tiles = planes[0].shape[1]
    smem, vmem = pl.BlockSpec(memory_space=pltpu.SMEM), pl.BlockSpec(memory_space=pltpu.VMEM)
    return pl.pallas_call(
        select_kernel,
        out_shape=[jax.ShapeDtypeStruct((PB, tiles, 16, 128), jnp.bfloat16)] * 4,
        in_specs=[smem] * 5 + [vmem] * 8,
        out_specs=[vmem] * 4,
        scratch_shapes=[pltpu.VMEM((8, 4, tiles, 16, 128), jnp.bfloat16)],
        interpret=INTERPRET,
        name="select",
    )(place, *pairs, *planes)


def cross_of(own, theirs, i):
    real, imag = None, None
    for (orr, oi), (pr, pi) in zip(own(i), theirs):
        real = add(real, orr * pr)
        real = add(real, oi * pi)
        imag = add(imag, orr * pi)
        imag = sub(imag, oi * pr)
    return real, imag


def correlate_kernel(h, place_ref, decay_ref, *refs):
    chunk, last = CHUNKS[h], h == len(CHUNKS) - 1
    refs = list(refs)
    take = lambda n: [refs.pop(0) for _ in range(n)]
    mine, theirs = take(4), take(4)
    (table_ref,) = take(1)
    (carry_ref, inverse_in) = take(2) if h else (None, None)
    outs = take(8) if last else take(2)
    own, cross, inverse, total = take(4)
    for r in range(4):
        own[r] = mine[r][...].astype(jnp.float32)

    def rows_of(tile, e_rows):
        def at(i):
            found = []
            for r in range(4):
                for e in e_rows:
                    re = own[r, tile + e, pl.ds(i, 1), :]
                    im = own[r, tile + e, pl.ds(8 + i, 1), :]
                    found.append((jnp.broadcast_to(re, (8, 128)), jnp.broadcast_to(im, (8, 128))))
            return found

        return at

    def partners(tile, k, e_rows):
        found = []
        for r in range(4):
            for e in e_rows:
                both = theirs[r][k, tile + e].astype(jnp.float32)
                found.append((both[:8], both[8:]))
        return found

    if h:
        inverse[...] = inverse_in[...]
    else:
        for k in range(PB):
            there = partners(2 * chunk, k, (0,))
            for i in range(LS):
                count = sum(
                    a * c + b * d for (a, b), (c, d) in zip(rows_of(2 * chunk, (0,))(i), there)
                )
                at = i * 32 + k * 8
                inverse[at : at + 8, :] = 1.0 / jnp.maximum(count, 1.0)

    for c in range(chunk):

        def per_slot(k, carry):
            there = partners(2 * c, k, (0, 1))
            for i in range(LS):
                real, imag = cross_of(rows_of(2 * c, (0, 1)), there, i)
                at = pl.ds(pl.multiple_of(i * 32 + k * 8, 8), 8)
                part = inverse[at, :]
                cross[at, 256 * c : 256 * c + 128] = real * part
                cross[at, 256 * c + 128 : 256 * (c + 1)] = imag * part
            return carry

        lax.fori_loop(0, PB, per_slot, 0)
    lagged = jnp.dot(
        cross[...].astype(jnp.bfloat16), table_ref[...], preferred_element_type=jnp.float32
    )
    if h:
        lagged = lagged + carry_ref[...]
    if not last:
        outs[0][...] = lagged
        outs[1][...] = inverse[...]
        return
    total[...] = lagged
    me = place_ref[2]
    decay = jnp.full((8, 128), decay_ref[0], jnp.float32)
    high = decay.astype(jnp.bfloat16)
    low = (decay - high.astype(jnp.float32)).astype(jnp.bfloat16)
    for r in range(8):
        at = pl.ds(pl.multiple_of((me ^ r) * 32, 32), 32)
        outs[r][:32, :] = total[at, :].astype(jnp.bfloat16)
        outs[r][32:40, :] = jnp.concatenate([high, low, jnp.zeros_like(low)], axis=1)


def correlate(h, place, decay, mine, theirs, table, carried):
    last = h == len(CHUNKS) - 1
    smem, vmem = pl.BlockSpec(memory_space=pltpu.SMEM), pl.BlockSpec(memory_space=pltpu.VMEM)
    if last:
        shapes = [jax.ShapeDtypeStruct((40, LAGS), jnp.bfloat16)] * 8
    else:
        shapes = [
            jax.ShapeDtypeStruct((256, LAGS), jnp.float32),
            jax.ShapeDtypeStruct((256, 128), jnp.float32),
        ]
    args = [*mine, *theirs, table, *carried]
    return pl.pallas_call(
        functools.partial(correlate_kernel, h),
        out_shape=shapes,
        in_specs=[smem] * 2 + [vmem] * len(args),
        out_specs=[vmem] * len(shapes),
        scratch_shapes=[
            pltpu.VMEM((4, tiles_of(h), 16, 128), jnp.float32),
            pltpu.VMEM((256, 256 * CHUNKS[h]), jnp.float32),
            pltpu.VMEM((256, 128), jnp.float32),
            pltpu.VMEM((256, LAGS), jnp.float32),
        ],
        interpret=INTERPRET,
        name=f"correlate{h}",
    )(place, decay, *args)


def scan_kernel(place_ref, *refs):
    ins, outs, (held, done) = refs[:8], refs[8:16], refs[16:]
    for r in range(8):
        held[r] = ins[r][...].astype(jnp.float32)
    me = place_ref[2]
    state = jnp.zeros((32, LAGS), jnp.float32)
    for w in range(8):
        slot = me ^ w
        decay = held[slot, 32:33, :128] + held[slot, 32:33, 128:256]
        decay = jnp.concatenate([decay] * 3, axis=1)
        state = decay * state + held[slot, :32, :]
        done[slot] = state
    for r in range(8):
        outs[r][...] = done[r].astype(jnp.bfloat16)


def scan_windows(place, ins):
    smem, vmem = pl.BlockSpec(memory_space=pltpu.SMEM), pl.BlockSpec(memory_space=pltpu.VMEM)
    return pl.pallas_call(
        scan_kernel,
        out_shape=[jax.ShapeDtypeStruct((32, LAGS), jnp.bfloat16)] * 8,
        in_specs=[smem] + [vmem] * 8,
        out_specs=[vmem] * 8,
        scratch_shapes=[
            pltpu.VMEM((8, 40, LAGS), jnp.float32),
            pltpu.VMEM((8, 32, LAGS), jnp.float32),
        ],
        interpret=INTERPRET,
        name="scan",
    )(place, *ins)


def gather_kernel(place_ref, *refs):
    ins, out = refs[:8], refs[8]
    me = place_ref[2]
    for r in range(8):
        out[me ^ r] = ins[r][...]


def gather_stations(place, ins):
    smem, vmem = pl.BlockSpec(memory_space=pltpu.SMEM), pl.BlockSpec(memory_space=pltpu.VMEM)
    return pl.pallas_call(
        gather_kernel,
        out_shape=jax.ShapeDtypeStruct((LS, 32, LAGS), jnp.bfloat16),
        in_specs=[smem] + [vmem] * 8,
        out_specs=vmem,
        interpret=INTERPRET,
        name="gather",
    )(place, *ins)


def across(value, axis, size, r):
    return lax.ppermute(value, axis, [(d, d ^ r) for d in range(size)])


def along(value, step):
    return lax.ppermute(value, "sta", [(d, (d + 4 * step) % 32) for d in range(32)])


def body(waveforms, segment_mask, pair_blocks, window_decay):
    here = lax.axis_index("sta")
    place = jnp.stack([here % 4, here // 4, lax.axis_index("section")]).astype(jnp.int32)
    pairs = [pair_blocks] + [across(pair_blocks, "sta", 32, r) for r in (1, 2, 3)]
    mask = jnp.broadcast_to(segment_mask.reshape(64, 1).astype(jnp.float32), (64, 128))
    count = len(CHUNKS)
    flat = spectrum(waveforms[0], mask, place)
    table = lag_table()
    carried, start = [], 0
    for h in range(count):
        mine = [flat[r * count + h] for r in range(4)]
        plane = [mine[0]] + [across(mine[r], "sta", 32, r) for r in (1, 2, 3)]
        plane = jnp.stack(plane)
        planes = [plane] + [None] * 7
        ahead = back = plane
        for step in range(1, 5):
            if step < 4 or h % 2 == 0:
                ahead = along(ahead, 1)
                planes[8 - step] = ahead
            if step < 4 or h % 2 == 1:
                back = along(back, -1)
                planes[step] = back
        chosen = select(place, pairs, planes)
        theirs = [chosen[0]] + [across(chosen[r], "sta", 32, r) for r in (1, 2, 3)]
        part = jnp.asarray(table[256 * start : 256 * (start + CHUNKS[h])])
        carried = correlate(h, place, window_decay, mine, theirs, part, carried)
        start += CHUNKS[h]
    ins = [carried[0]] + [across(carried[r], "section", 8, r) for r in range(1, 8)]
    outs = scan_windows(place, ins)
    outs = [outs[0]] + [across(outs[r], "section", 8, r) for r in range(1, 8)]
    return gather_stations(place, outs)[None]


def solution(mesh):
    placed = (
        P("section", "sta", None, None),
        P("section", "sta", None),
        P("sta", None),
        P("section"),
    )
    return jax.shard_map(
        body, mesh=mesh, in_specs=placed, out_specs=P("section", "sta", None, None), check_vma=False
    )
```

```python
import functools
import math

import jax
import jax.numpy as jnp
import numpy as np
from jax import lax
from jax.experimental import pallas as pl
from jax.experimental.pallas import tpu as pltpu
from jax.sharding import PartitionSpec as P


NF = 1024
LAGS = 384
NSAMP = 4096
LS = 8
SEGS = 8
PB = 4
EPSILON = 1e-05
CHUNKS = (5, 3)


def twiddles():
    k = np.arange(32)[:, None]
    b = np.arange(128)[None, :]
    angle = 2.0 * np.pi * (k * b) / NSAMP
    return np.stack([np.cos(angle), np.sin(angle)]).astype(np.float32)


def second_dft():
    b = np.arange(128)[:, None]
    m = np.arange(4, 36)[None, :]
    angle = 2.0 * np.pi * ((b * m) % 128) / 128
    cos, sin = np.cos(angle) / 64, np.sin(angle) / 64
    full = np.zeros((256, 256))
    full[:128, :32] = cos
    full[128:, :32] = sin
    full[:128, 128:160] = -sin
    full[128:, 128:160] = cos
    high = full.astype(jnp.bfloat16)
    low = (full - high.astype(np.float64)).astype(jnp.bfloat16)
    return np.stack([high, low])


def lag_table():
    freq = 128 + np.arange(NF)
    shift = np.arange(LAGS) + NSAMP - LAGS // 2
    phase = (freq[:, None] * shift[None, :] % NSAMP).astype(np.float32)
    phase = phase * np.float32(2.0 * np.pi / NSAMP)
    cos = np.cos(phase) / np.float32(math.sqrt(NF))
    sin = -np.sin(phase) / np.float32(math.sqrt(NF))
    lane = np.arange(128)
    rows = []
    for c in range(8):
        f = 8 * (lane // 32) + c + 32 * (lane % 32)
        rows += [cos[f], sin[f]]
    return np.concatenate(rows).reshape(8, 256, LAGS).astype(jnp.bfloat16)


def add(a, b):
    return b if a is None else a if b is None else a + b


def sub(a, b):
    if b is None:
        return a
    return -b if a is None else a - b


def real_fft(xs):
    n = len(xs)
    if n == 1:
        return [(xs[0], None)]
    if n == 2:
        return [(xs[0] + xs[1], None), (xs[0] - xs[1], None)]
    even, odd = real_fft(xs[0::2]), real_fft(xs[1::2])
    out = [None] * (n // 2 + 1)
    for k in range(n // 4 + 1):
        (er, ei), (orr, oi) = even[k], odd[k]
        if k == 0:
            tr, ti = orr, oi
        elif 4 * k == n:
            tr, ti = oi, None if orr is None else -orr
        else:
            c, s = math.cos(2 * math.pi * k / n), math.sin(2 * math.pi * k / n)
            if oi is None:
                tr, ti = orr * c, orr * (-s)
            else:
                tr, ti = orr * c + oi * s, oi * c - orr * s
        out[k] = (add(er, tr), add(ei, ti))
        out[n // 2 - k] = (sub(er, tr), sub(ti, ei))
    return out


def spots():
    here = lax.axis_index("sta")
    return here % 4, here // 4, lax.axis_index("section")


def spectrum_kernel(mask_ref, wave_ref, turn_ref, dft_ref, *refs):
    outs, (mid, bins, white, marks) = refs[:-4], refs[-4:]

    def station(i, carry):
        xs = [wave_ref[i, :, 128 * a : 128 * (a + 1)].astype(jnp.float32) for a in range(32)]
        half = real_fft(xs)
        for k in range(32):
            re, im = half[k] if k <= 16 else half[32 - k]
            if k > 16 and im is not None:
                im = -im
            if k:
                cos, sin = turn_ref[0, k : k + 1, :], turn_ref[1, k : k + 1, :]
                if im is None:
                    re, im = re * cos, -(re * sin)
                else:
                    re, im = re * cos + im * sin, im * cos - re * sin
            klo, c = divmod(k, 8)
            rows = pl.ds(pl.multiple_of(c * 64 + i * 8, 8), 8)
            mid[klo, rows, :128] = re
            mid[klo, rows, 128:] = jnp.zeros_like(re) if im is None else im
        seg = lax.broadcasted_iota(jnp.int32, (SEGS, 128), 0)
        mark = jnp.zeros((SEGS, 128), jnp.float32)
        for e in range(SEGS):
            mark = jnp.where(seg == e, mask_ref[0, i, e].astype(jnp.float32), mark)
        marks[pl.ds(pl.multiple_of(i * 8, 8), 8), :] = mark
        return carry

    lax.fori_loop(0, LS, station, 0)
    dot = functools.partial(jnp.dot, preferred_element_type=jnp.float32)
    bins[...] = jnp.zeros_like(bins)

    def second(klo, carry):
        weights = []
        for part in range(2):
            base = dft_ref[part].astype(jnp.float32)
            sides = [pltpu.roll(base[:, at : at + 128], 32 * klo, 1) for at in (0, 128)]
            weights.append(jnp.concatenate(sides, axis=1).astype(jnp.bfloat16))
        wh, wl = weights
        value = mid[klo]
        high = value.astype(jnp.bfloat16)
        low = (value - high.astype(jnp.float32)).astype(jnp.bfloat16)
        bins[...] += dot(high, wh) + (dot(low, wh) + dot(high, wl))
        return carry

    lax.fori_loop(0, 4, second, 0)
    re, im = bins[:, :128], bins[:, 128:]
    amp = jnp.sqrt(re * re + im * im)
    amps = [amp[64 * c : 64 * (c + 1)] for c in range(8)]
    before, after = [amps[0]], [amps[7]]
    for c in range(1, 8):
        before.append(before[-1] + amps[c])
        after.append(after[-1] + amps[7 - c])
    after = after[::-1]
    total = before[7]
    lane = lax.broadcasted_iota(jnp.int32, (64, 128), 1)
    klo = lane // 32
    m = lane % 32
    turned = [pltpu.roll(total, 32 * d, 1) for d in (1, 2, 3)]
    zero = jnp.zeros_like(total)
    all_klo = total + turned[0] + turned[1] + turned[2]
    lower = upper = zero
    for d in (1, 2, 3):
        lower = lower + jnp.where(klo >= d, turned[d - 1], zero)
        upper = upper + jnp.where(klo + d <= 3, turned[3 - d], zero)
    for c in range(8):
        left = pltpu.roll(after[c] + upper, 1, 1)
        right = pltpu.roll(before[c] + lower, 127, 1)
        smooth = all_klo + jnp.where(m >= 1, left, zero) + jnp.where(m <= 30, right, zero)
        scale = marks[...] / (smooth * (1.0 / 65) + EPSILON)
        rows = slice(64 * c, 64 * (c + 1))
        white[0, rows, :] = re[rows] * scale
        white[1, rows, :] = im[rows] * scale
    place = spots()[0]
    count = len(CHUNKS)
    for r in range(4):
        for e in range(2):
            seg = 2 * (place ^ r) + e
            c = 0
            for h in range(count):
                out = outs[r * count + h]
                for local in range(CHUNKS[h]):
                    at = pl.ds(64 * c + seg, 8, stride=8)
                    tile = jnp.concatenate([white[0, at, :], white[1, at, :]], axis=0)
                    out[2 * local + e] = tile.astype(jnp.bfloat16)
                    c += 1
        seg = 2 * (place ^ r)
        tile = [marks[pl.ds(seg + e, 8, stride=8), :] for e in range(2)]
        outs[r * count][2 * CHUNKS[0]] = jnp.concatenate(tile, axis=0).astype(jnp.bfloat16)


def tiles_of(h):
    return 2 * CHUNKS[h] + (h == 0)


def spectrum(waves, mask):
    shapes = [
        jax.ShapeDtypeStruct((tiles_of(h), 16, 128), jnp.bfloat16)
        for _ in range(4)
        for h in range(len(CHUNKS))
    ]
    vmem = pl.BlockSpec(memory_space=pltpu.VMEM)
    return pl.pallas_call(
        spectrum_kernel,
        out_shape=shapes,
        in_specs=[pl.BlockSpec(memory_space=pltpu.SMEM)] + [vmem] * 3,
        out_specs=[vmem] * len(shapes),
        scratch_shapes=[
            pltpu.VMEM((4, 512, 256), jnp.float32),
            pltpu.VMEM((512, 256), jnp.float32),
            pltpu.VMEM((2, 512, 128), jnp.float32),
            pltpu.VMEM((64, 128), jnp.float32),
        ],
        name="spectrum",
    )(mask, waves, jnp.asarray(twiddles()), jnp.asarray(second_dft()))


def select_kernel(*refs):
    pairs, planes, outs, held = refs[:4], refs[4:12], refs[12:16], refs[16]
    for dz in range(8):
        held[dz] = planes[dz][...]
    mate, z, _ = spots()
    for r in range(4):
        for k in range(PB):
            p = pairs[r][0, k]
            dz = ((p // 4) - z + 8) % 8
            outs[r][k] = held[dz, (p % 4) ^ mate]


def select(pairs, planes):
    tiles = planes[0].shape[1]
    smem, vmem = pl.BlockSpec(memory_space=pltpu.SMEM), pl.BlockSpec(memory_space=pltpu.VMEM)
    return pl.pallas_call(
        select_kernel,
        out_shape=[jax.ShapeDtypeStruct((PB, tiles, 16, 128), jnp.bfloat16)] * 4,
        in_specs=[smem] * 4 + [vmem] * 8,
        out_specs=[vmem] * 4,
        scratch_shapes=[pltpu.VMEM((8, 4, tiles, 16, 128), jnp.bfloat16)],
        name="select",
    )(*pairs, *planes)


def cross_of(own, theirs, i):
    real, imag = None, None
    for (orr, oi), (pr, pi) in zip(own(i), theirs):
        real = add(real, orr * pr)
        real = add(real, oi * pi)
        imag = add(imag, orr * pi)
        imag = sub(imag, oi * pr)
    return real, imag


def correlate_kernel(h, decay_ref, *refs):
    chunk, last = CHUNKS[h], h == len(CHUNKS) - 1
    refs = list(refs)
    take = lambda n: [refs.pop(0) for _ in range(n)]
    mine, theirs = take(4), take(4)
    (table_ref,) = take(1)
    (carry_ref, inverse_in) = take(2) if h else (None, None)
    outs = take(4) if last else take(2)
    own, cross, inverse, total = take(4)
    for r in range(4):
        own[r] = mine[r][...].astype(jnp.float32)

    def rows_of(tile, e_rows):
        def at(i):
            found = []
            for r in range(4):
                for e in e_rows:
                    re = own[r, tile + e, pl.ds(i, 1), :]
                    im = own[r, tile + e, pl.ds(8 + i, 1), :]
                    found.append((jnp.broadcast_to(re, (8, 128)), jnp.broadcast_to(im, (8, 128))))
            return found

        return at

    def partners(tile, k, e_rows):
        found = []
        for r in range(4):
            for e in e_rows:
                both = theirs[r][k, tile + e].astype(jnp.float32)
                found.append((both[:8], both[8:]))
        return found

    if h:
        inverse[...] = inverse_in[...]
    else:
        for k in range(PB):
            there = partners(2 * chunk, k, (0,))
            for i in range(LS):
                count = sum(
                    a * c + b * d for (a, b), (c, d) in zip(rows_of(2 * chunk, (0,))(i), there)
                )
                at = i * 32 + k * 8
                inverse[at : at + 8, :] = 1.0 / jnp.maximum(count, 1.0)

    def per_slot(step, carry):
        c, k = step // PB, step % PB
        there = partners(2 * c, k, (0, 1))
        for i in range(LS):
            real, imag = cross_of(rows_of(2 * c, (0, 1)), there, i)
            at = pl.ds(pl.multiple_of(i * 32 + k * 8, 8), 8)
            part = inverse[at, :]
            cross[c, at, :128] = real * part
            cross[c, at, 128:] = imag * part
        return carry

    lax.fori_loop(0, chunk * PB, per_slot, 0)
    total[...] = carry_ref[...] if h else jnp.zeros_like(total)

    def per_row(c, carry):
        spectra = cross[c].astype(jnp.bfloat16)
        total[...] += jnp.dot(spectra, table_ref[c], preferred_element_type=jnp.float32)
        return carry

    lax.fori_loop(0, chunk, per_row, 0)
    if not last:
        outs[0][...] = total[...]
        outs[1][...] = inverse[...]
        return
    x = spots()[2] % 4
    decay = jnp.full((8, 128), decay_ref[0], jnp.float32)
    high = decay.astype(jnp.bfloat16)
    low = (decay - high.astype(jnp.float32)).astype(jnp.bfloat16)
    for r in range(4):
        at = pl.ds(pl.multiple_of((x ^ r) * 64, 64), 64)
        outs[r][:64, :] = total[at, :].astype(jnp.bfloat16)
        outs[r][64:72, :] = jnp.concatenate([high, low, jnp.zeros_like(low)], axis=1)


def correlate(h, decay, mine, theirs, table, carried):
    last = h == len(CHUNKS) - 1
    smem, vmem = pl.BlockSpec(memory_space=pltpu.SMEM), pl.BlockSpec(memory_space=pltpu.VMEM)
    if last:
        shapes = [jax.ShapeDtypeStruct((72, LAGS), jnp.bfloat16)] * 4
    else:
        shapes = [
            jax.ShapeDtypeStruct((256, LAGS), jnp.float32),
            jax.ShapeDtypeStruct((256, 128), jnp.float32),
        ]
    args = [*mine, *theirs, table, *carried]
    return pl.pallas_call(
        functools.partial(correlate_kernel, h),
        out_shape=shapes,
        in_specs=[smem] + [vmem] * len(args),
        out_specs=[vmem] * len(shapes),
        scratch_shapes=[
            pltpu.VMEM((4, tiles_of(h), 16, 128), jnp.float32),
            pltpu.VMEM((CHUNKS[h], 256, 256), jnp.float32),
            pltpu.VMEM((256, 128), jnp.float32),
            pltpu.VMEM((256, LAGS), jnp.float32),
        ],
    )(decay, *args)


def scan_kernel(rescan, *refs):
    ins, outs, (held, done) = refs[:4], refs[4:-2], refs[-2:]
    for r in range(4):
        held[r] = ins[r][...].astype(jnp.float32)
    x = spots()[2] % 4
    if rescan:
        state, outs = outs[0][...].astype(jnp.float32), outs[1:]
    else:
        state = jnp.zeros((64, LAGS), jnp.float32)
    for w in range(4):
        slot = x ^ w
        decay = held[slot, 64:65, :128] + held[slot, 64:65, 128:256]
        decay = jnp.concatenate([decay] * 3, axis=1)
        state = decay * state + held[slot, :64, :]
        if rescan:
            done[slot] = state
    if not rescan:
        outs[0][...] = state.astype(jnp.bfloat16)
        return
    for r in range(4):
        outs[r][...] = done[r].astype(jnp.bfloat16)


def scan_windows(ins, entering):
    vmem = pl.BlockSpec(memory_space=pltpu.VMEM)
    count = 4 if entering else 1
    return pl.pallas_call(
        functools.partial(scan_kernel, bool(entering)),
        out_shape=[jax.ShapeDtypeStruct((64, LAGS), jnp.bfloat16)] * count,
        in_specs=[vmem] * (4 + len(entering)),
        out_specs=[vmem] * count,
        scratch_shapes=[
            pltpu.VMEM((4, 72, LAGS), jnp.float32),
            pltpu.VMEM((4, 64, LAGS), jnp.float32),
        ],
        name="rescan" if entering else "scan",
    )(*ins, *entering)


def gather_kernel(*refs):
    ins, out = refs[:4], refs[4]
    x = spots()[2] % 4
    for r in range(4):
        out[x ^ r] = ins[r][...]


def gather_stations(ins):
    vmem = pl.BlockSpec(memory_space=pltpu.VMEM)
    return pl.pallas_call(
        gather_kernel,
        out_shape=jax.ShapeDtypeStruct((4, 64, LAGS), jnp.bfloat16),
        in_specs=[vmem] * 4,
        out_specs=vmem,
        name="gather",
    )(*ins)


def across(value, axis, size, r):
    return lax.ppermute(value, axis, [(d, d ^ r) for d in range(size)])


def along(value, step):
    return lax.ppermute(value, "sta", [(d, (d + 4 * step) % 32) for d in range(32)])


def body(waveforms, segment_mask, pair_blocks, window_decay):
    pairs = [pair_blocks] + [across(pair_blocks, "sta", 32, r) for r in (1, 2, 3)]
    count = len(CHUNKS)
    flat = spectrum(waveforms[0], segment_mask)
    table = lag_table()
    carried, start = [], 0
    for h in range(count):
        mine = [flat[r * count + h] for r in range(4)]
        plane = [mine[0]] + [across(mine[r], "sta", 32, r) for r in (1, 2, 3)]
        plane = jnp.stack(plane)
        planes = [plane] + [None] * 7
        ahead = back = plane
        for step in range(1, 5):
            if step < 4 or h % 2 == 0:
                ahead = along(ahead, 1)
                planes[8 - step] = ahead
            if step < 4 or h % 2 == 1:
                back = along(back, -1)
                planes[step] = back
        chosen = select(pairs, planes)
        theirs = [across(chosen[r], "sta", 32, r) for r in (1, 2, 3)]
        part = jnp.asarray(table[start : start + CHUNKS[h]])
        carried = correlate(h, window_decay, mine, [chosen[0], *theirs], part, carried)
        start += CHUNKS[h]
    ins = [carried[0]] + [across(carried[r], "section", 8, r) for r in (1, 2, 3)]
    (total,) = scan_windows(ins, [])
    entering = lax.ppermute(total, "section", [(d, d + 4) for d in range(4)])
    outs = scan_windows(ins, [entering])
    outs = [outs[0]] + [across(outs[r], "section", 8, r) for r in (1, 2, 3)]
    return gather_stations(outs).reshape(1, LS, 32, LAGS)


def solution(mesh):
    placed = (
        P("section", "sta", None, None),
        P("section", "sta", None),
        P("sta", None),
        P("section"),
    )

    return jax.shard_map(
        body, mesh=mesh, in_specs=placed, out_specs=P("section", "sta", None, None), check_vma=False
    )
```

```python
import functools
import math

import jax
import jax.numpy as jnp
import numpy as np
from jax import lax
from jax.experimental import pallas as pl
from jax.experimental.pallas import tpu as pltpu
from jax.sharding import Mesh
from jax.sharding import PartitionSpec as P


NF = 1024
LAGS = 384
NSAMP = 4096
LS = 8
SEGS = 8
PB = 4
EPSILON = 1e-05
HALVES = 2


def twiddles():
    k = np.arange(32)[:, None]
    b = np.arange(128)[None, :]
    angle = 2.0 * np.pi * (k * b) / NSAMP
    return np.stack([np.cos(angle), np.sin(angle)]).astype(np.float32)


def second_dft():
    b = np.arange(128)[:, None]
    m = np.arange(4, 36)[None, :]
    angle = 2.0 * np.pi * ((b * m) % 128) / 128
    cos, sin = np.cos(angle) / 64, np.sin(angle) / 64
    full = np.zeros((256, 256))
    full[:128, :32] = cos
    full[128:, :32] = sin
    full[:128, 128:160] = -sin
    full[128:, 128:160] = cos
    high = full.astype(jnp.bfloat16)
    low = (full - high.astype(np.float64)).astype(jnp.bfloat16)
    return np.stack([high, low])


def lag_table():
    freq = 128 + np.arange(NF)
    shift = np.arange(LAGS) + NSAMP - LAGS // 2
    phase = (freq[:, None] * shift[None, :] % NSAMP).astype(np.float32)
    phase = phase * np.float32(2.0 * np.pi / NSAMP)
    cos = np.cos(phase) / np.float32(math.sqrt(NF))
    sin = -np.sin(phase) / np.float32(math.sqrt(NF))
    lane = np.arange(128)
    rows = []
    for c in range(8):
        f = 8 * (lane // 32) + c + 32 * (lane % 32)
        rows += [cos[f], sin[f]]
    return np.concatenate(rows).reshape(8, 256, LAGS).astype(jnp.bfloat16)


def add(a, b):
    return b if a is None else a if b is None else a + b


def sub(a, b):
    if b is None:
        return a
    return -b if a is None else a - b


def real_fft(xs):
    n = len(xs)
    if n == 1:
        return [(xs[0], None)]
    if n == 2:
        return [(xs[0] + xs[1], None), (xs[0] - xs[1], None)]
    even, odd = real_fft(xs[0::2]), real_fft(xs[1::2])
    out = [None] * (n // 2 + 1)
    for k in range(n // 4 + 1):
        (er, ei), (orr, oi) = even[k], odd[k]
        if k == 0:
            tr, ti = orr, oi
        elif 4 * k == n:
            tr, ti = oi, None if orr is None else -orr
        else:
            c, s = math.cos(2 * math.pi * k / n), math.sin(2 * math.pi * k / n)
            if oi is None:
                tr, ti = orr * c, orr * (-s)
            else:
                tr, ti = orr * c + oi * s, oi * c - orr * s
        out[k] = (add(er, tr), add(ei, ti))
        out[n // 2 - k] = (sub(er, tr), sub(ti, ei))
    return out


def spots():
    return lax.axis_index("section"), lax.axis_index("z"), lax.axis_index("mate")


def spectrum_kernel(mask_ref, wave_ref, turn_ref, dft_ref, *refs):
    outs, (mid, bins, white, marks) = refs[:-4], refs[-4:]
    lane_at = lax.broadcasted_iota(jnp.int32, (LS, 128), 1)
    row_at = lax.broadcasted_iota(jnp.int32, (LS, 128), 0)

    def station(i, carry):
        xs = [wave_ref[i, :, 128 * a : 128 * (a + 1)].astype(jnp.float32) for a in range(32)]
        half = real_fft(xs)
        for k in range(32):
            re, im = half[k] if k <= 16 else half[32 - k]
            if k > 16 and im is not None:
                im = -im
            if k:
                cos, sin = turn_ref[0, k : k + 1, :], turn_ref[1, k : k + 1, :]
                if im is None:
                    re, im = re * cos, -(re * sin)
                else:
                    re, im = re * cos + im * sin, im * cos - re * sin
            klo, c = divmod(k, 8)
            rows = pl.ds(pl.multiple_of(c * 64 + i * 8, 8), 8)
            mid[klo, rows, :128] = re
            mid[klo, rows, 128:] = jnp.zeros_like(re) if im is None else im
        mark = jnp.zeros((SEGS, 128), jnp.float32)
        for e in range(SEGS):
            valid = mask_ref[0, i, e].astype(jnp.float32)
            mark = jnp.where(row_at == e, valid, mark)
            carry = jnp.where((row_at == i) & (lane_at == e), valid, carry)
        marks[pl.ds(pl.multiple_of(i * 8, 8), 8), :] = mark
        return carry

    table = lax.fori_loop(0, LS, station, jnp.zeros((LS, 128), jnp.float32))
    dot = functools.partial(jnp.dot, preferred_element_type=jnp.float32)
    bins[...] = jnp.zeros_like(bins)

    def second(klo, carry):
        weights = []
        for part in range(2):
            base = dft_ref[part].astype(jnp.float32)
            sides = [pltpu.roll(base[:, at : at + 128], 32 * klo, 1) for at in (0, 128)]
            weights.append(jnp.concatenate(sides, axis=1).astype(jnp.bfloat16))
        wh, wl = weights
        value = mid[klo]
        high = value.astype(jnp.bfloat16)
        low = (value - high.astype(jnp.float32)).astype(jnp.bfloat16)
        bins[...] += dot(high, wh) + (dot(low, wh) + dot(high, wl))
        return carry

    lax.fori_loop(0, 4, second, 0)
    re, im = bins[:, :128], bins[:, 128:]
    amp = jnp.sqrt(re * re + im * im)
    amps = [amp[64 * c : 64 * (c + 1)] for c in range(8)]
    before, after = [amps[0]], [amps[7]]
    for c in range(1, 8):
        before.append(before[-1] + amps[c])
        after.append(after[-1] + amps[7 - c])
    after = after[::-1]
    total = before[7]
    lane = lax.broadcasted_iota(jnp.int32, (64, 128), 1)
    klo = lane // 32
    m = lane % 32
    turned = [pltpu.roll(total, 32 * d, 1) for d in (1, 2, 3)]
    zero = jnp.zeros_like(total)
    all_klo = total + turned[0] + turned[1] + turned[2]
    lower = upper = zero
    for d in (1, 2, 3):
        lower = lower + jnp.where(klo >= d, turned[d - 1], zero)
        upper = upper + jnp.where(klo + d <= 3, turned[3 - d], zero)
    for c in range(8):
        left = pltpu.roll(after[c] + upper, 1, 1)
        right = pltpu.roll(before[c] + lower, 127, 1)
        smooth = all_klo + jnp.where(m >= 1, left, zero) + jnp.where(m <= 30, right, zero)
        scale = marks[...] / (smooth * (1.0 / 65) + EPSILON)
        rows = slice(64 * c, 64 * (c + 1))
        white[0, rows, :] = re[rows] * scale
        white[1, rows, :] = im[rows] * scale
    mate = spots()[2]
    for r in range(4):
        for h in range(HALVES):
            out = outs[r * HALVES + h]
            first = 64 * (2 * (mate ^ r) + h)
            for seg in range(SEGS):
                at = pl.ds(first + seg, 8, stride=8)
                tile = jnp.concatenate([white[0, at, :], white[1, at, :]], axis=0)
                out[16 * seg : 16 * seg + 16, :] = tile.astype(jnp.bfloat16)
        outs[r * HALVES][128:136, :] = table.astype(jnp.bfloat16)


def rows_of(h):
    return 128 + 8 * (h == 0)


def spectrum(waves, mask):
    shapes = [
        jax.ShapeDtypeStruct((rows_of(h), 128), jnp.bfloat16)
        for _ in range(4)
        for h in range(HALVES)
    ]
    vmem = pl.BlockSpec(memory_space=pltpu.VMEM)
    return pl.pallas_call(
        spectrum_kernel,
        out_shape=shapes,
        in_specs=[pl.BlockSpec(memory_space=pltpu.SMEM)] + [vmem] * 3,
        out_specs=[vmem] * len(shapes),
        scratch_shapes=[
            pltpu.VMEM((4, 512, 256), jnp.float32),
            pltpu.VMEM((512, 256), jnp.float32),
            pltpu.VMEM((2, 512, 128), jnp.float32),
            pltpu.VMEM((64, 128), jnp.float32),
        ],
        name="spectrum",
    )(mask, waves, jnp.asarray(twiddles()), jnp.asarray(second_dft()))


def correlate_kernel(h, decay_ref, *refs):
    last = h == HALVES - 1
    refs = list(refs)
    take = lambda n: [refs.pop(0) for _ in range(n)]
    pairs, planes = take(4), take(8)
    (table_hbm,) = take(1)
    before = take(2) if h else None
    outs = take(1) if last else take(2)
    held, cross, inverse, total, table, sem = take(6)
    _, z, mate = spots()
    fetch = pltpu.make_async_copy(table_hbm.at[2 * mate + h], table, sem)
    fetch.start()
    for dz in range(8):
        for r in range(4):
            held[4 * dz + r] = planes[dz][r].astype(jnp.float32)

    def block_of(q, k):
        p = pairs[0][0, k]
        for r in range(1, 4):
            p = jnp.where((q ^ mate) == r, pairs[r][0, k], p)
        dz = ((p // 4) - z + 8) % 8
        return 4 * dz + ((p % 4) ^ mate)

    def out_rows(i, q, k):
        return pl.ds(pl.multiple_of(i * 128 + q * 32 + k * 8, 8), 8)

    if h:
        inverse[...] = before[1][...]
    else:

        def per_count(step, carry):
            q, k = step // PB, step % PB
            there = held[block_of(q, k), 128:136, :]
            for i in range(LS):
                here = held[q ^ mate, 128 + i : 129 + i, :]
                inverse[out_rows(i, q, k), :] = here * there
            return carry

        lax.fori_loop(0, 4 * PB, per_count, 0)
        ones = jnp.ones((128, 128), jnp.bfloat16)
        count = jnp.dot(
            inverse[...].astype(jnp.bfloat16), ones, preferred_element_type=jnp.float32
        )
        inverse[...] = 1.0 / jnp.maximum(count, 1.0)

    def per_pair(step, carry):
        q, k = step // PB, step % PB
        theirs, mine = block_of(q, k), q ^ mate
        there = [held[theirs, 8 * e : 8 * e + 8, :] for e in range(2 * SEGS)]
        for i in range(LS):
            real, imag = None, None
            for e in range(SEGS):
                pr, pi = there[2 * e], there[2 * e + 1]
                at = 16 * e + i
                mr = jnp.broadcast_to(held[mine, at : at + 1, :], (8, 128))
                mi = jnp.broadcast_to(held[mine, at + 8 : at + 9, :], (8, 128))
                real = add(real, mr * pr)
                real = add(real, mi * pi)
                imag = add(imag, mr * pi)
                imag = sub(imag, mi * pr)
            at = out_rows(i, q, k)
            part = inverse[at, :]
            cross[at, :128] = real * part
            cross[at, 128:] = imag * part
        return carry

    lax.fori_loop(0, 4 * PB, per_pair, 0)
    fetch.wait()

    def per_rows(step, carry):
        at = pl.ds(pl.multiple_of(step * 256, 256), 256)
        spectra = cross[at, :].astype(jnp.bfloat16)
        part = jnp.dot(spectra, table[...], preferred_element_type=jnp.float32)
        total[at, :] = part + before[0][at, :] if h else part
        return carry

    lax.fori_loop(0, 4, per_rows, 0)
    if not last:
        outs[0][...] = total[...]
        outs[1][...] = inverse[...]
        return
    decay = jnp.full((8, 128), decay_ref[0], jnp.float32)
    high = decay.astype(jnp.bfloat16)
    low = (decay - high.astype(jnp.float32)).astype(jnp.bfloat16)
    both = jnp.where(row_of(8) < 4, high.astype(jnp.float32), low.astype(jnp.float32))

    def per_part(n, carry):
        at = pl.ds(pl.multiple_of(n * 32, 32), 32)
        for g in range(3):
            value = total[at, 128 * g : 128 * (g + 1)]
            outs[0][n, 32 * g : 32 * (g + 1), :] = value.astype(jnp.bfloat16)
        outs[0][n, 96:104, :] = both.astype(jnp.bfloat16)
        return carry

    lax.fori_loop(0, 32, per_part, 0)


def row_of(n):
    return lax.broadcasted_iota(jnp.int32, (n, 128), 0)


def correlate(h, decay, pairs, planes, table, carried):
    last = h == HALVES - 1
    smem, vmem = pl.BlockSpec(memory_space=pltpu.SMEM), pl.BlockSpec(memory_space=pltpu.VMEM)
    if last:
        shapes = [jax.ShapeDtypeStruct((32, 104, 128), jnp.bfloat16)]
    else:
        shapes = [
            jax.ShapeDtypeStruct((1024, LAGS), jnp.float32),
            jax.ShapeDtypeStruct((1024, 128), jnp.float32),
        ]
    return pl.pallas_call(
        functools.partial(correlate_kernel, h),
        out_shape=shapes,
        in_specs=[smem] * 5
        + [vmem] * 8
        + [pl.BlockSpec(memory_space=pl.ANY)]
        + [vmem] * len(carried),
        out_specs=[vmem] * len(shapes),
        scratch_shapes=[
            pltpu.VMEM((32, rows_of(h), 128), jnp.float32),
            pltpu.VMEM((1024, 256), jnp.float32),
            pltpu.VMEM((1024, 128), jnp.float32),
            pltpu.VMEM((1024, LAGS), jnp.float32),
            pltpu.VMEM((256, LAGS), jnp.bfloat16),
            pltpu.SemaphoreType.DMA,
        ],
    )(decay, *pairs, *planes, table, *carried)


def scan_kernel(parts, out):
    state = [jnp.zeros((32, 128), jnp.float32)] * 3
    for w in range(8):
        marks = parts[4 * w, 96:104, :].astype(jnp.float32)
        decay = marks[:1] + marks[4:5]
        for g in range(3):
            at = slice(32 * g, 32 * (g + 1))
            lagged = sum(parts[4 * w + q, at, :].astype(jnp.float32) for q in range(4))
            state[g] = decay * state[g] + lagged
            out[w, :, 128 * g : 128 * (g + 1)] = state[g].astype(jnp.bfloat16)


def scan_windows(parts):
    vmem = pl.BlockSpec(memory_space=pltpu.VMEM)
    return pl.pallas_call(
        scan_kernel,
        out_shape=jax.ShapeDtypeStruct((8, 32, LAGS), jnp.bfloat16),
        in_specs=[vmem],
        out_specs=vmem,
        name="scan",
    )(parts)


def across(value, r):
    return lax.ppermute(value, "mate", [(d, d ^ r) for d in range(4)])


def along(value, step):
    return lax.ppermute(value, "z", [(d, (d + step) % 8) for d in range(8)])


def body(waveforms, segment_mask, pair_blocks, window_decay):
    pairs = [pair_blocks] + [across(pair_blocks, r) for r in (1, 2, 3)]
    flat = spectrum(waveforms[0], segment_mask)
    table = jnp.asarray(lag_table())
    carried = []
    for h in range(HALVES):
        mine = [flat[r * HALVES + h] for r in range(4)]
        plane = jnp.stack([mine[0]] + [across(mine[r], r) for r in (1, 2, 3)])
        planes = [plane] + [None] * 7
        ahead = back = plane
        for step in range(1, 5):
            if step < 4 or h % 2 == 0:
                ahead = along(ahead, 1)
                planes[8 - step] = ahead
            if step < 4 or h % 2 == 1:
                back = along(back, -1)
                planes[step] = back
        carried = correlate(h, window_decay, pairs, planes, table, carried)
    parts = lax.all_to_all(carried[0], ("section", "mate"), 0, 0)
    states = lax.all_to_all(scan_windows(parts), "section", 0, 0)
    return states[None]


def solution(mesh):
    split = Mesh(mesh.devices.reshape(8, 8, 4), ("section", "z", "mate"))
    sta = ("z", "mate")
    placed = (P("section", sta, None, None), P("section", sta, None), P(sta, None), P("section"))

    return jax.shard_map(
        body,
        mesh=split,
        in_specs=placed,
        out_specs=P("section", sta, None, None),
        check_vma=False,
    )
```

```python
import functools
import math

import jax
import jax.numpy as jnp
import numpy as np
from jax import lax
from jax.experimental import pallas as pl
from jax.experimental.pallas import tpu as pltpu
from jax.sharding import Mesh
from jax.sharding import PartitionSpec as P


NF = 1024
LAGS = 384
NSAMP = 4096
LS = 8
SEGS = 8
PB = 4
EPSILON = 1e-05
HALVES = 2


def twiddles():
    k = np.arange(32)[:, None]
    b = np.arange(128)[None, :]
    angle = 2.0 * np.pi * (k * b) / NSAMP
    return np.stack([np.cos(angle), np.sin(angle)]).astype(np.float32)


def second_dft():
    b = np.arange(128)[:, None]
    m = np.arange(4, 36)[None, :]
    angle = 2.0 * np.pi * ((b * m) % 128) / 128
    cos, sin = np.cos(angle) / 64, np.sin(angle) / 64
    full = np.zeros((256, 256))
    full[:128, :32] = cos
    full[128:, :32] = sin
    full[:128, 128:160] = -sin
    full[128:, 128:160] = cos
    high = full.astype(jnp.bfloat16)
    low = (full - high.astype(np.float64)).astype(jnp.bfloat16)
    return np.stack([high, low])


def lag_table():
    freq = 128 + np.arange(NF)
    shift = np.arange(LAGS) + NSAMP - LAGS // 2
    phase = (freq[:, None] * shift[None, :] % NSAMP).astype(np.float32)
    phase = phase * np.float32(2.0 * np.pi / NSAMP)
    cos = np.cos(phase) / np.float32(math.sqrt(NF))
    sin = -np.sin(phase) / np.float32(math.sqrt(NF))
    lane = np.arange(128)
    rows = []
    for c in range(8):
        f = 8 * (lane // 32) + c + 32 * (lane % 32)
        rows += [cos[f], sin[f]]
    return np.concatenate(rows).reshape(8, 256, LAGS).astype(jnp.bfloat16)


def add(a, b):
    return b if a is None else a if b is None else a + b


def sub(a, b):
    if b is None:
        return a
    return -b if a is None else a - b


def real_fft(xs):
    n = len(xs)
    if n == 1:
        return [(xs[0], None)]
    if n == 2:
        return [(xs[0] + xs[1], None), (xs[0] - xs[1], None)]
    even, odd = real_fft(xs[0::2]), real_fft(xs[1::2])
    out = [None] * (n // 2 + 1)
    for k in range(n // 4 + 1):
        (er, ei), (orr, oi) = even[k], odd[k]
        if k == 0:
            tr, ti = orr, oi
        elif 4 * k == n:
            tr, ti = oi, None if orr is None else -orr
        else:
            c, s = math.cos(2 * math.pi * k / n), math.sin(2 * math.pi * k / n)
            if oi is None:
                tr, ti = orr * c, orr * (-s)
            else:
                tr, ti = orr * c + oi * s, oi * c - orr * s
        out[k] = (add(er, tr), add(ei, ti))
        out[n // 2 - k] = (sub(er, tr), sub(ti, ei))
    return out


def spots():
    return lax.axis_index("section"), lax.axis_index("z"), lax.axis_index("mate")


def spectrum_kernel(mask_ref, wave_ref, turn_ref, dft_ref, *refs):
    outs, (mid, bins, white, marks) = refs[:-4], refs[-4:]
    lane_at = lax.broadcasted_iota(jnp.int32, (LS, 128), 1)
    row_at = lax.broadcasted_iota(jnp.int32, (LS, 128), 0)

    def station(i, carry):
        xs = [wave_ref[i, :, 128 * a : 128 * (a + 1)].astype(jnp.float32) for a in range(32)]
        half = real_fft(xs)
        for k in range(32):
            re, im = half[k] if k <= 16 else half[32 - k]
            if k > 16 and im is not None:
                im = -im
            if k:
                cos, sin = turn_ref[0, k : k + 1, :], turn_ref[1, k : k + 1, :]
                if im is None:
                    re, im = re * cos, -(re * sin)
                else:
                    re, im = re * cos + im * sin, im * cos - re * sin
            klo, c = divmod(k, 8)
            rows = pl.ds(pl.multiple_of(c * 64 + i * 8, 8), 8)
            mid[klo, rows, :128] = re
            mid[klo, rows, 128:] = jnp.zeros_like(re) if im is None else im
        mark = jnp.zeros((SEGS, 128), jnp.float32)
        for e in range(SEGS):
            valid = mask_ref[0, i, e].astype(jnp.float32)
            mark = jnp.where(row_at == e, valid, mark)
            carry = jnp.where((row_at == i) & (lane_at == e), valid, carry)
        marks[pl.ds(pl.multiple_of(i * 8, 8), 8), :] = mark
        return carry

    table = lax.fori_loop(0, LS, station, jnp.zeros((LS, 128), jnp.float32))
    dot = functools.partial(jnp.dot, preferred_element_type=jnp.float32)
    bins[...] = jnp.zeros_like(bins)

    def second(klo, carry):
        weights = []
        for part in range(2):
            base = dft_ref[part].astype(jnp.float32)
            sides = [pltpu.roll(base[:, at : at + 128], 32 * klo, 1) for at in (0, 128)]
            weights.append(jnp.concatenate(sides, axis=1).astype(jnp.bfloat16))
        wh, wl = weights
        value = mid[klo]
        high = value.astype(jnp.bfloat16)
        low = (value - high.astype(jnp.float32)).astype(jnp.bfloat16)
        bins[...] += dot(high, wh) + (dot(low, wh) + dot(high, wl))
        return carry

    lax.fori_loop(0, 4, second, 0)
    re, im = bins[:, :128], bins[:, 128:]
    amp = jnp.sqrt(re * re + im * im)
    amps = [amp[64 * c : 64 * (c + 1)] for c in range(8)]
    before, after = [amps[0]], [amps[7]]
    for c in range(1, 8):
        before.append(before[-1] + amps[c])
        after.append(after[-1] + amps[7 - c])
    after = after[::-1]
    total = before[7]
    lane = lax.broadcasted_iota(jnp.int32, (64, 128), 1)
    klo = lane // 32
    m = lane % 32
    turned = [pltpu.roll(total, 32 * d, 1) for d in (1, 2, 3)]
    zero = jnp.zeros_like(total)
    all_klo = total + turned[0] + turned[1] + turned[2]
    lower = upper = zero
    for d in (1, 2, 3):
        lower = lower + jnp.where(klo >= d, turned[d - 1], zero)
        upper = upper + jnp.where(klo + d <= 3, turned[3 - d], zero)
    for c in range(8):
        left = pltpu.roll(after[c] + upper, 1, 1)
        right = pltpu.roll(before[c] + lower, 127, 1)
        smooth = all_klo + jnp.where(m >= 1, left, zero) + jnp.where(m <= 30, right, zero)
        scale = marks[...] / (smooth * (1.0 / 65) + EPSILON)
        rows = slice(64 * c, 64 * (c + 1))
        white[0, rows, :] = re[rows] * scale
        white[1, rows, :] = im[rows] * scale
    mate = spots()[2]
    for r in range(4):
        for h in range(HALVES):
            out = outs[r * HALVES + h]
            first = 64 * (2 * (mate ^ r) + h)
            for seg in range(SEGS):
                at = pl.ds(first + seg, 8, stride=8)
                tile = jnp.concatenate([white[0, at, :], white[1, at, :]], axis=0)
                out[16 * seg : 16 * seg + 16, :] = tile.astype(jnp.bfloat16)
        outs[r * HALVES + HALVES - 1][128:136, :] = table.astype(jnp.bfloat16)


def rows_of(h):
    return 128 + 8 * (h == HALVES - 1)


def spectrum(waves, mask):
    shapes = [
        jax.ShapeDtypeStruct((rows_of(h), 128), jnp.bfloat16)
        for _ in range(4)
        for h in range(HALVES)
    ]
    vmem = pl.BlockSpec(memory_space=pltpu.VMEM)
    return pl.pallas_call(
        spectrum_kernel,
        out_shape=shapes,
        in_specs=[pl.BlockSpec(memory_space=pltpu.SMEM)] + [vmem] * 3,
        out_specs=[vmem] * len(shapes),
        scratch_shapes=[
            pltpu.VMEM((4, 512, 256), jnp.float32),
            pltpu.VMEM((512, 256), jnp.float32),
            pltpu.VMEM((2, 512, 128), jnp.float32),
            pltpu.VMEM((64, 128), jnp.float32),
        ],
        name="spectrum",
    )(mask, waves, jnp.asarray(twiddles()), jnp.asarray(second_dft()))


def correlate_kernel(h, decay_ref, *refs):
    last = h == HALVES - 1
    refs = list(refs)
    take = lambda n: [refs.pop(0) for _ in range(n)]
    pairs, planes = take(4), take(8)
    (table_hbm,) = take(1)
    before = take(1)[0] if h else None
    (out,) = take(1)
    held, cross, total, inverse, table, spot, sem = take(7)
    _, z, mate = spots()
    fetch = pltpu.make_async_copy(table_hbm.at[2 * mate + h], table, sem)
    fetch.start()
    for r in range(4):
        for k in range(PB):
            p = pairs[r][0, k]
            dz = ((p // 4) - z + 8) % 8
            spot[(mate ^ r) * PB + k] = 4 * dz + ((p % 4) ^ mate)
    for dz in range(8):
        for r in range(4):
            held[4 * dz + r] = planes[dz][r].astype(jnp.float32)

    def per_pair(step, carry):
        q, k = step // PB, step % PB
        theirs, mine = spot[step], q ^ mate
        there = [held[theirs, 8 * e : 8 * e + 8, :] for e in range(2 * SEGS)]
        if last:
            marks = held[theirs, 128:136, :]
        for i in range(LS):
            real, imag = None, None
            for e in range(SEGS):
                pr, pi = there[2 * e], there[2 * e + 1]
                at = 16 * e + i
                mr = jnp.broadcast_to(held[mine, at : at + 1, :], (8, 128))
                mi = jnp.broadcast_to(held[mine, at + 8 : at + 9, :], (8, 128))
                real = add(real, mr * pr)
                real = add(real, mi * pi)
                imag = add(imag, mr * pi)
                imag = sub(imag, mi * pr)
            at = pl.ds(pl.multiple_of(i * 128 + q * 32 + k * 8, 8), 8)
            cross[at, :128] = real
            cross[at, 128:] = imag
            if last:
                inverse[at, :] = held[mine, 128 + i : 129 + i, :] * marks
        return carry

    lax.fori_loop(0, 4 * PB, per_pair, 0)
    if last:
        ones = jnp.ones((128, 128), jnp.bfloat16)
        count = jnp.dot(
            inverse[...].astype(jnp.bfloat16), ones, preferred_element_type=jnp.float32
        )
        inverse[...] = 1.0 / jnp.maximum(count, 1.0)
    fetch.wait()
    lagged = total if last else out

    def per_rows(step, carry):
        at = pl.ds(pl.multiple_of(step * 256, 256), 256)
        spectra = cross[at, :].astype(jnp.bfloat16)
        part = jnp.dot(spectra, table[...], preferred_element_type=jnp.float32)
        lagged[at, :] = part + before[at, :] if h else part
        return carry

    lax.fori_loop(0, 4, per_rows, 0)
    if not last:
        return
    decay = jnp.full((8, 128), decay_ref[0], jnp.float32)
    high = decay.astype(jnp.bfloat16)
    low = (decay - high.astype(jnp.float32)).astype(jnp.bfloat16)
    both = jnp.where(row_of(8) < 4, high.astype(jnp.float32), low.astype(jnp.float32))

    def per_part(n, carry):
        at = pl.ds(pl.multiple_of(n * 32, 32), 32)
        part = inverse[at, :]
        for g in range(3):
            value = total[at, 128 * g : 128 * (g + 1)] * part
            out[n, 32 * g : 32 * (g + 1), :] = value.astype(jnp.bfloat16)
        out[n, 96:104, :] = both.astype(jnp.bfloat16)
        return carry

    lax.fori_loop(0, 32, per_part, 0)


def row_of(n):
    return lax.broadcasted_iota(jnp.int32, (n, 128), 0)


def correlate(h, decay, pairs, planes, table, carried):
    last = h == HALVES - 1
    smem, vmem = pl.BlockSpec(memory_space=pltpu.SMEM), pl.BlockSpec(memory_space=pltpu.VMEM)
    if last:
        shapes = [jax.ShapeDtypeStruct((32, 104, 128), jnp.bfloat16)]
    else:
        shapes = [jax.ShapeDtypeStruct((1024, LAGS), jnp.float32)]
    return pl.pallas_call(
        functools.partial(correlate_kernel, h),
        out_shape=shapes,
        in_specs=[smem] * 5
        + [vmem] * 8
        + [pl.BlockSpec(memory_space=pl.ANY)]
        + [vmem] * len(carried),
        out_specs=[vmem] * len(shapes),
        scratch_shapes=[
            pltpu.VMEM((32, rows_of(h), 128), jnp.float32),
            pltpu.VMEM((1024, 256), jnp.float32),
            pltpu.VMEM((1024 if last else 8, LAGS), jnp.float32),
            pltpu.VMEM((1024 if last else 8, 128), jnp.float32),
            pltpu.VMEM((256, LAGS), jnp.bfloat16),
            pltpu.SMEM((4 * PB,), jnp.int32),
            pltpu.SemaphoreType.DMA,
        ],
    )(decay, *pairs, *planes, table, *carried)


def scan_kernel(parts, out):
    state = [jnp.zeros((32, 128), jnp.float32)] * 3
    for w in range(8):
        marks = parts[4 * w, 96:104, :].astype(jnp.float32)
        decay = marks[:1] + marks[4:5]
        for g in range(3):
            at = slice(32 * g, 32 * (g + 1))
            lagged = sum(parts[4 * w + q, at, :].astype(jnp.float32) for q in range(4))
            state[g] = decay * state[g] + lagged
            out[w, :, 128 * g : 128 * (g + 1)] = state[g].astype(jnp.bfloat16)


def scan_windows(parts):
    vmem = pl.BlockSpec(memory_space=pltpu.VMEM)
    return pl.pallas_call(
        scan_kernel,
        out_shape=jax.ShapeDtypeStruct((8, 32, LAGS), jnp.bfloat16),
        in_specs=[vmem],
        out_specs=vmem,
        name="scan",
    )(parts)


def across(value, r):
    return lax.ppermute(value, "mate", [(d, d ^ r) for d in range(4)])


def along(value, step):
    return lax.ppermute(value, "z", [(d, (d + step) % 8) for d in range(8)])


def body(waveforms, segment_mask, pair_blocks, window_decay):
    pairs = [pair_blocks] + [across(pair_blocks, r) for r in (1, 2, 3)]
    flat = spectrum(waveforms[0], segment_mask)
    table = jnp.asarray(lag_table())
    carried = []
    for h in range(HALVES):
        mine = [flat[r * HALVES + h] for r in range(4)]
        plane = jnp.stack([mine[0]] + [across(mine[r], r) for r in (1, 2, 3)])
        planes = [plane] + [None] * 7
        ahead = back = plane
        for step in range(1, 5):
            if step < 4 or h % 2 == 0:
                ahead = along(ahead, 1)
                planes[8 - step] = ahead
            if step < 4 or h % 2 == 1:
                back = along(back, -1)
                planes[step] = back
        carried = correlate(h, window_decay, pairs, planes, table, carried)
    parts = lax.all_to_all(carried[0], ("section", "mate"), 0, 0)
    states = lax.all_to_all(scan_windows(parts), "section", 0, 0)
    return states[None]


def solution(mesh):
    split = Mesh(mesh.devices.reshape(8, 8, 4), ("section", "z", "mate"))
    sta = ("z", "mate")
    placed = (P("section", sta, None, None), P("section", sta, None), P(sta, None), P("section"))

    return jax.shard_map(
        body,
        mesh=split,
        in_specs=placed,
        out_specs=P("section", sta, None, None),
        check_vma=False,
    )
```

```python
import functools
import math

import jax
import jax.numpy as jnp
import numpy as np
from jax import lax
from jax.experimental import pallas as pl
from jax.experimental.pallas import tpu as pltpu
from jax.sharding import Mesh
from jax.sharding import PartitionSpec as P


NF = 1024
LAGS = 384
NSAMP = 4096
LS = 8
SEGS = 8
PB = 4
EPSILON = 1e-05
HALVES = 2


def twiddles():
    k = np.arange(32)[:, None]
    b = np.arange(128)[None, :]
    angle = 2.0 * np.pi * (k * b) / NSAMP
    return np.stack([np.cos(angle), np.sin(angle)]).astype(np.float32)


def second_dft():
    b = np.arange(128)[:, None]
    m = np.arange(4, 36)[None, :]
    angle = 2.0 * np.pi * ((b * m) % 128) / 128
    cos, sin = np.cos(angle) / 64, np.sin(angle) / 64
    full = np.zeros((256, 256))
    full[:128, :32] = cos
    full[128:, :32] = sin
    full[:128, 128:160] = -sin
    full[128:, 128:160] = cos
    high = full.astype(jnp.bfloat16)
    low = (full - high.astype(np.float64)).astype(jnp.bfloat16)
    return np.stack([high, low])


def lag_table():
    freq = 128 + np.arange(NF)
    shift = np.arange(LAGS) + NSAMP - LAGS // 2
    phase = (freq[:, None] * shift[None, :] % NSAMP).astype(np.float32)
    phase = phase * np.float32(2.0 * np.pi / NSAMP)
    cos = np.cos(phase) / np.float32(math.sqrt(NF))
    sin = -np.sin(phase) / np.float32(math.sqrt(NF))
    lane = np.arange(128)
    rows = []
    for c in range(8):
        f = 8 * (lane // 32) + c + 32 * (lane % 32)
        rows += [cos[f], sin[f]]
    return np.concatenate(rows).reshape(8, 256, LAGS).astype(jnp.bfloat16)


def add(a, b):
    return b if a is None else a if b is None else a + b


def sub(a, b):
    if b is None:
        return a
    return -b if a is None else a - b


def real_fft(xs):
    n = len(xs)
    if n == 1:
        return [(xs[0], None)]
    if n == 2:
        return [(xs[0] + xs[1], None), (xs[0] - xs[1], None)]
    even, odd = real_fft(xs[0::2]), real_fft(xs[1::2])
    out = [None] * (n // 2 + 1)
    for k in range(n // 4 + 1):
        (er, ei), (orr, oi) = even[k], odd[k]
        if k == 0:
            tr, ti = orr, oi
        elif 4 * k == n:
            tr, ti = oi, None if orr is None else -orr
        else:
            c, s = math.cos(2 * math.pi * k / n), math.sin(2 * math.pi * k / n)
            if oi is None:
                tr, ti = orr * c, orr * (-s)
            else:
                tr, ti = orr * c + oi * s, oi * c - orr * s
        out[k] = (add(er, tr), add(ei, ti))
        out[n // 2 - k] = (sub(er, tr), sub(ti, ei))
    return out


def spots():
    return lax.axis_index("z"), 2 * lax.axis_index("y") + lax.axis_index("c")


def spectrum_kernel(mask_ref, wave_ref, turn_ref, dft_ref, *refs):
    outs, (mid, bins, white, marks) = refs[:-4], refs[-4:]
    lane_at = lax.broadcasted_iota(jnp.int32, (LS, 128), 1)
    row_at = lax.broadcasted_iota(jnp.int32, (LS, 128), 0)

    def station(i, carry):
        xs = [wave_ref[i, :, 128 * a : 128 * (a + 1)].astype(jnp.float32) for a in range(32)]
        half = real_fft(xs)
        for k in range(32):
            re, im = half[k] if k <= 16 else half[32 - k]
            if k > 16 and im is not None:
                im = -im
            if k:
                cos, sin = turn_ref[0, k : k + 1, :], turn_ref[1, k : k + 1, :]
                if im is None:
                    re, im = re * cos, -(re * sin)
                else:
                    re, im = re * cos + im * sin, im * cos - re * sin
            klo, c = divmod(k, 8)
            rows = pl.ds(pl.multiple_of(c * 64 + i * 8, 8), 8)
            mid[klo, rows, :128] = re
            mid[klo, rows, 128:] = jnp.zeros_like(re) if im is None else im
        mark = jnp.zeros((SEGS, 128), jnp.float32)
        for e in range(SEGS):
            valid = mask_ref[0, i, e].astype(jnp.float32)
            mark = jnp.where(row_at == e, valid, mark)
            carry = jnp.where((row_at == i) & (lane_at == e), valid, carry)
        marks[pl.ds(pl.multiple_of(i * 8, 8), 8), :] = mark
        return carry

    table = lax.fori_loop(0, LS, station, jnp.zeros((LS, 128), jnp.float32))
    dot = functools.partial(jnp.dot, preferred_element_type=jnp.float32)
    bins[...] = jnp.zeros_like(bins)

    def second(klo, carry):
        weights = []
        for part in range(2):
            base = dft_ref[part].astype(jnp.float32)
            sides = [pltpu.roll(base[:, at : at + 128], 32 * klo, 1) for at in (0, 128)]
            weights.append(jnp.concatenate(sides, axis=1).astype(jnp.bfloat16))
        wh, wl = weights
        value = mid[klo]
        high = value.astype(jnp.bfloat16)
        low = (value - high.astype(jnp.float32)).astype(jnp.bfloat16)
        bins[...] += dot(high, wh) + (dot(low, wh) + dot(high, wl))
        return carry

    lax.fori_loop(0, 4, second, 0)
    re, im = bins[:, :128], bins[:, 128:]
    amp = jnp.sqrt(re * re + im * im)
    amps = [amp[64 * c : 64 * (c + 1)] for c in range(8)]
    before, after = [amps[0]], [amps[7]]
    for c in range(1, 8):
        before.append(before[-1] + amps[c])
        after.append(after[-1] + amps[7 - c])
    after = after[::-1]
    total = before[7]
    lane = lax.broadcasted_iota(jnp.int32, (64, 128), 1)
    klo = lane // 32
    m = lane % 32
    turned = [pltpu.roll(total, 32 * d, 1) for d in (1, 2, 3)]
    zero = jnp.zeros_like(total)
    all_klo = total + turned[0] + turned[1] + turned[2]
    lower = upper = zero
    for d in (1, 2, 3):
        lower = lower + jnp.where(klo >= d, turned[d - 1], zero)
        upper = upper + jnp.where(klo + d <= 3, turned[3 - d], zero)
    for c in range(8):
        left = pltpu.roll(after[c] + upper, 1, 1)
        right = pltpu.roll(before[c] + lower, 127, 1)
        smooth = all_klo + jnp.where(m >= 1, left, zero) + jnp.where(m <= 30, right, zero)
        scale = marks[...] / (smooth * (1.0 / 65) + EPSILON)
        rows = slice(64 * c, 64 * (c + 1))
        white[0, rows, :] = re[rows] * scale
        white[1, rows, :] = im[rows] * scale
    mate = spots()[1]
    for r in range(4):
        for h in range(HALVES):
            out = outs[r * HALVES + h]
            first = 64 * (2 * (mate ^ r) + h)
            for seg in range(SEGS):
                at = pl.ds(first + seg, 8, stride=8)
                tile = jnp.concatenate([white[0, at, :], white[1, at, :]], axis=0)
                out[16 * seg : 16 * seg + 16, :] = tile.astype(jnp.bfloat16)
        outs[r * HALVES + HALVES - 1][128:136, :] = table.astype(jnp.bfloat16)


def rows_of(h):
    return 128 + 8 * (h == HALVES - 1)


def spectrum(waves, mask):
    shapes = [
        jax.ShapeDtypeStruct((rows_of(h), 128), jnp.bfloat16)
        for _ in range(4)
        for h in range(HALVES)
    ]
    vmem = pl.BlockSpec(memory_space=pltpu.VMEM)
    return pl.pallas_call(
        spectrum_kernel,
        out_shape=shapes,
        in_specs=[pl.BlockSpec(memory_space=pltpu.SMEM)] + [vmem] * 3,
        out_specs=[vmem] * len(shapes),
        scratch_shapes=[
            pltpu.VMEM((4, 512, 256), jnp.float32),
            pltpu.VMEM((512, 256), jnp.float32),
            pltpu.VMEM((2, 512, 128), jnp.float32),
            pltpu.VMEM((64, 128), jnp.float32),
        ],
        name="spectrum",
    )(mask, waves, jnp.asarray(twiddles()), jnp.asarray(second_dft()))


def correlate_kernel(h, decay_ref, *refs):
    last = h == HALVES - 1
    refs = list(refs)
    take = lambda n: [refs.pop(0) for _ in range(n)]
    pairs, planes = take(4), take(8)
    (table_hbm,) = take(1)
    before = take(1)[0] if h else None
    outs = take(2) if last else take(1)
    held, own, cross, total, inverse, table, spot, plane_sem, sem = take(9)
    z, mate = spots()
    loads = [
        pltpu.make_async_copy(planes[dz], held.at[pl.ds(4 * dz, 4)], plane_sem.at[dz])
        for dz in range(8)
    ]
    fetches = [pltpu.make_async_copy(table_hbm.at[2 * mate + h], table, sem.at[0])]
    if h:
        fetches.append(pltpu.make_async_copy(before, total, sem.at[1]))
    for copy in loads + fetches:
        copy.start()
    for r in range(4):
        for k in range(PB):
            p = pairs[r][0, k]
            dz = ((p // 4) - z + 8) % 8
            spot[(mate ^ r) * PB + k] = 4 * dz + ((p % 4) ^ mate)
    loads[0].wait()
    for r in range(4):
        own[r] = held[r].astype(jnp.float32)
    for copy in loads[1:]:
        copy.wait()

    def per_pair(step, carry):
        q, k = step // PB, step % PB
        theirs, mine = spot[step], q ^ mate
        tiles = [held[theirs, 16 * e : 16 * e + 16, :].astype(jnp.float32) for e in range(SEGS)]
        if last:
            marks = held[theirs, 128:136, :].astype(jnp.float32)
        for i in range(LS):
            real, imag = None, None
            for e in range(SEGS):
                pr, pi = tiles[e][:8], tiles[e][8:]
                at = 16 * e + i
                mr = jnp.broadcast_to(own[mine, at : at + 1, :], (8, 128))
                mi = jnp.broadcast_to(own[mine, at + 8 : at + 9, :], (8, 128))
                real = add(real, mr * pr)
                real = add(real, mi * pi)
                imag = add(imag, mr * pi)
                imag = sub(imag, mi * pr)
            at = pl.ds(pl.multiple_of(i * 128 + q * 32 + k * 8, 8), 8)
            cross[at, :128] = real
            cross[at, 128:] = imag
            if last:
                inverse[at, :] = own[mine, 128 + i : 129 + i, :] * marks
        return carry

    lax.fori_loop(0, 4 * PB, per_pair, 0)
    if last:
        ones = jnp.ones((128, 128), jnp.bfloat16)
        count = jnp.dot(
            inverse[...].astype(jnp.bfloat16), ones, preferred_element_type=jnp.float32
        )
        inverse[...] = 1.0 / jnp.maximum(count, 1.0)
    for copy in fetches:
        copy.wait()
    lagged = total if last else outs[0]

    def per_rows(step, carry):
        at = pl.ds(pl.multiple_of(step * 256, 256), 256)
        spectra = cross[at, :].astype(jnp.bfloat16)
        part = jnp.dot(spectra, table[...], preferred_element_type=jnp.float32)
        lagged[at, :] = part + lagged[at, :] if h else part
        return carry

    lax.fori_loop(0, 4, per_rows, 0)
    if not last:
        return
    decay = jnp.full((8, 128), decay_ref[0], jnp.float32)
    high = decay.astype(jnp.bfloat16)
    low = (decay - high.astype(jnp.float32)).astype(jnp.bfloat16)
    both = jnp.where(row_of(8) < 4, high.astype(jnp.float32), low.astype(jnp.float32))

    core = mate % 2

    def per_part(n, carry):
        i, y = n // 2, n % 2
        for keep in range(2):
            q = 2 * y + (core ^ keep)
            at = pl.ds(pl.multiple_of(i * 128 + q * 32, 32), 32)
            part = inverse[at, :]
            for g in range(3):
                value = total[at, 128 * g : 128 * (g + 1)] * part
                outs[keep][n, 32 * g : 32 * (g + 1), :] = value.astype(jnp.bfloat16)
            marks = jnp.zeros_like(both) if keep else both
            outs[keep][n, 96:104, :] = marks.astype(jnp.bfloat16)
        return carry

    lax.fori_loop(0, 16, per_part, 0)


def row_of(n):
    return lax.broadcasted_iota(jnp.int32, (n, 128), 0)


def correlate(h, decay, pairs, planes, table, carried):
    last = h == HALVES - 1
    smem, vmem = pl.BlockSpec(memory_space=pltpu.SMEM), pl.BlockSpec(memory_space=pltpu.VMEM)
    if last:
        shapes = [jax.ShapeDtypeStruct((16, 104, 128), jnp.bfloat16)] * 2
    else:
        shapes = [jax.ShapeDtypeStruct((1024, LAGS), jnp.float32)]
    return pl.pallas_call(
        functools.partial(correlate_kernel, h),
        out_shape=shapes,
        in_specs=[smem] * 5
        + [pl.BlockSpec(memory_space=pl.ANY)] * (9 + len(carried)),
        out_specs=[vmem] * len(shapes),
        scratch_shapes=[
            pltpu.VMEM((32, rows_of(h), 128), jnp.bfloat16),
            pltpu.VMEM((4, rows_of(h), 128), jnp.float32),
            pltpu.VMEM((1024, 256), jnp.float32),
            pltpu.VMEM((1024 if last else 8, LAGS), jnp.float32),
            pltpu.VMEM((1024 if last else 8, 128), jnp.float32),
            pltpu.VMEM((256, LAGS), jnp.bfloat16),
            pltpu.SMEM((4 * PB,), jnp.int32),
            pltpu.SemaphoreType.DMA((8,)),
            pltpu.SemaphoreType.DMA((2,)),
        ],
    )(decay, *pairs, *planes, table, *carried)


def scan_kernel(parts, out):
    state = [jnp.zeros((32, 128), jnp.float32)] * 3
    for w in range(8):
        marks = parts[2 * w, 96:104, :].astype(jnp.float32)
        decay = marks[:1] + marks[4:5]
        for g in range(3):
            at = slice(32 * g, 32 * (g + 1))
            lagged = parts[2 * w, at, :].astype(jnp.float32)
            lagged = lagged + parts[2 * w + 1, at, :].astype(jnp.float32)
            state[g] = decay * state[g] + lagged
            out[w, :, 128 * g : 128 * (g + 1)] = state[g].astype(jnp.bfloat16)


def scan_windows(parts):
    vmem = pl.BlockSpec(memory_space=pltpu.VMEM)
    return pl.pallas_call(
        scan_kernel,
        out_shape=jax.ShapeDtypeStruct((8, 32, LAGS), jnp.bfloat16),
        in_specs=[vmem],
        out_specs=vmem,
        name="scan",
    )(parts)


def across(value, r):
    return lax.ppermute(value, ("y", "c"), [(d, d ^ r) for d in range(4)])


def along(value, step):
    return lax.ppermute(value, "z", [(d, (d + step) % 8) for d in range(8)])


def body(waveforms, segment_mask, pair_blocks, window_decay):
    pairs = [pair_blocks] + [across(pair_blocks, r) for r in (1, 2, 3)]
    flat = spectrum(waveforms[0], segment_mask)
    table = jnp.asarray(lag_table())
    carried = []
    for h in range(HALVES):
        mine = [flat[r * HALVES + h] for r in range(4)]
        plane = jnp.stack([mine[0]] + [across(mine[r], r) for r in (1, 2, 3)])
        planes = [plane] + [None] * 7
        ahead = back = plane
        for step in range(1, 5):
            if step < 4 or h % 2 == 0:
                ahead = along(ahead, 1)
                planes[8 - step] = ahead
            if step < 4 or h % 2 == 1:
                back = along(back, -1)
                planes[step] = back
        carried = correlate(h, window_decay, pairs, planes, table, carried)
    kept, sent = carried
    kept = kept.astype(jnp.float32) + across(sent, 1).astype(jnp.float32)
    parts = lax.all_to_all(kept.astype(jnp.bfloat16), ("section", "y"), 0, 0)
    states = lax.all_to_all(scan_windows(parts), "section", 0, 0)
    return states[None]


def solution(mesh):
    split = Mesh(mesh.devices.reshape(8, 8, 2, 2), ("section", "z", "y", "c"))
    sta = ("z", "y", "c")
    placed = (P("section", sta, None, None), P("section", sta, None), P(sta, None), P("section"))

    return jax.shard_map(
        body,
        mesh=split,
        in_specs=placed,
        out_specs=P("section", sta, None, None),
        check_vma=False,
    )
```

```python
import functools
import math

import jax
import jax.numpy as jnp
import numpy as np
from jax import lax
from jax.experimental import pallas as pl
from jax.experimental.pallas import tpu as pltpu
from jax.sharding import Mesh
from jax.sharding import PartitionSpec as P


NF = 1024
LAGS = 384
NSAMP = 4096
LS = 8
SEGS = 8
PB = 4
EPSILON = 1e-05
HALVES = 2


def twiddles():
    k = np.arange(32)[:, None]
    b = np.arange(128)[None, :]
    angle = 2.0 * np.pi * (k * b) / NSAMP
    return np.stack([np.cos(angle), np.sin(angle)]).astype(np.float32)


def second_dft():
    b = np.arange(128)[:, None]
    m = np.arange(4, 36)[None, :]
    angle = 2.0 * np.pi * ((b * m) % 128) / 128
    cos, sin = np.cos(angle) / 64, np.sin(angle) / 64
    full = np.zeros((256, 256))
    full[:128, :32] = cos
    full[128:, :32] = sin
    full[:128, 128:160] = -sin
    full[128:, 128:160] = cos
    high = full.astype(jnp.bfloat16)
    low = (full - high.astype(np.float64)).astype(jnp.bfloat16)
    return np.stack([high, low])


def lag_table():
    freq = 128 + np.arange(NF)
    shift = np.arange(LAGS) + NSAMP - LAGS // 2
    phase = (freq[:, None] * shift[None, :] % NSAMP).astype(np.float32)
    phase = phase * np.float32(2.0 * np.pi / NSAMP)
    cos = np.cos(phase) / np.float32(math.sqrt(NF))
    sin = -np.sin(phase) / np.float32(math.sqrt(NF))
    lane = np.arange(128)
    rows = []
    for c in range(8):
        f = 8 * (lane // 32) + c + 32 * (lane % 32)
        rows += [cos[f], sin[f]]
    return np.concatenate(rows).reshape(8, 256, LAGS).astype(jnp.bfloat16)


def add(a, b):
    return b if a is None else a if b is None else a + b


def sub(a, b):
    if b is None:
        return a
    return -b if a is None else a - b


def real_fft(xs):
    n = len(xs)
    if n == 1:
        return [(xs[0], None)]
    if n == 2:
        return [(xs[0] + xs[1], None), (xs[0] - xs[1], None)]
    even, odd = real_fft(xs[0::2]), real_fft(xs[1::2])
    out = [None] * (n // 2 + 1)
    for k in range(n // 4 + 1):
        (er, ei), (orr, oi) = even[k], odd[k]
        if k == 0:
            tr, ti = orr, oi
        elif 4 * k == n:
            tr, ti = oi, None if orr is None else -orr
        else:
            c, s = math.cos(2 * math.pi * k / n), math.sin(2 * math.pi * k / n)
            if oi is None:
                tr, ti = orr * c, orr * (-s)
            else:
                tr, ti = orr * c + oi * s, oi * c - orr * s
        out[k] = (add(er, tr), add(ei, ti))
        out[n // 2 - k] = (sub(er, tr), sub(ti, ei))
    return out


def spots():
    return lax.axis_index("z"), 2 * lax.axis_index("y") + lax.axis_index("c")


def spectrum_kernel(mask_ref, wave_ref, turn_ref, dft_ref, *refs):
    outs, (mid, bins, white, marks) = refs[:-4], refs[-4:]
    lane_at = lax.broadcasted_iota(jnp.int32, (LS, 128), 1)
    row_at = lax.broadcasted_iota(jnp.int32, (LS, 128), 0)

    def station(i, carry):
        xs = [wave_ref[i, :, 128 * a : 128 * (a + 1)].astype(jnp.float32) for a in range(32)]
        half = real_fft(xs)
        for k in range(32):
            re, im = half[k] if k <= 16 else half[32 - k]
            if k > 16 and im is not None:
                im = -im
            if k:
                cos, sin = turn_ref[0, k : k + 1, :], turn_ref[1, k : k + 1, :]
                if im is None:
                    re, im = re * cos, -(re * sin)
                else:
                    re, im = re * cos + im * sin, im * cos - re * sin
            klo, c = divmod(k, 8)
            rows = pl.ds(pl.multiple_of(c * 64 + i * 8, 8), 8)
            mid[klo, rows, :128] = re
            mid[klo, rows, 128:] = jnp.zeros_like(re) if im is None else im
        mark = jnp.zeros((SEGS, 128), jnp.float32)
        for e in range(SEGS):
            valid = mask_ref[0, i, e].astype(jnp.float32)
            mark = jnp.where(row_at == e, valid, mark)
            carry = jnp.where((row_at == i) & (lane_at == e), valid, carry)
        marks[pl.ds(pl.multiple_of(i * 8, 8), 8), :] = mark
        return carry

    table = lax.fori_loop(0, LS, station, jnp.zeros((LS, 128), jnp.float32))
    dot = functools.partial(jnp.dot, preferred_element_type=jnp.float32)
    bins[...] = jnp.zeros_like(bins)

    def second(klo, carry):
        weights = []
        for part in range(2):
            base = dft_ref[part].astype(jnp.float32)
            sides = [pltpu.roll(base[:, at : at + 128], 32 * klo, 1) for at in (0, 128)]
            weights.append(jnp.concatenate(sides, axis=1).astype(jnp.bfloat16))
        wh, wl = weights
        value = mid[klo]
        high = value.astype(jnp.bfloat16)
        low = (value - high.astype(jnp.float32)).astype(jnp.bfloat16)
        bins[...] += dot(high, wh) + (dot(low, wh) + dot(high, wl))
        return carry

    lax.fori_loop(0, 4, second, 0)
    re, im = bins[:, :128], bins[:, 128:]
    amp = jnp.sqrt(re * re + im * im)
    amps = [amp[64 * c : 64 * (c + 1)] for c in range(8)]
    before, after = [amps[0]], [amps[7]]
    for c in range(1, 8):
        before.append(before[-1] + amps[c])
        after.append(after[-1] + amps[7 - c])
    after = after[::-1]
    total = before[7]
    lane = lax.broadcasted_iota(jnp.int32, (64, 128), 1)
    klo = lane // 32
    m = lane % 32
    turned = [pltpu.roll(total, 32 * d, 1) for d in (1, 2, 3)]
    zero = jnp.zeros_like(total)
    all_klo = total + turned[0] + turned[1] + turned[2]
    lower = upper = zero
    for d in (1, 2, 3):
        lower = lower + jnp.where(klo >= d, turned[d - 1], zero)
        upper = upper + jnp.where(klo + d <= 3, turned[3 - d], zero)
    for c in range(8):
        left = pltpu.roll(after[c] + upper, 1, 1)
        right = pltpu.roll(before[c] + lower, 127, 1)
        smooth = all_klo + jnp.where(m >= 1, left, zero) + jnp.where(m <= 30, right, zero)
        scale = marks[...] / (smooth * (1.0 / 65) + EPSILON)
        rows = slice(64 * c, 64 * (c + 1))
        white[0, rows, :] = re[rows] * scale
        white[1, rows, :] = im[rows] * scale
    mate = spots()[1]
    for r in range(4):
        for h in range(HALVES):
            out = outs[r * HALVES + h]
            first = 64 * (2 * (mate ^ r) + h)
            for seg in range(SEGS):
                at = pl.ds(first + seg, 8, stride=8)
                tile = jnp.concatenate([white[0, at, :], white[1, at, :]], axis=0)
                out[16 * seg : 16 * seg + 16, :] = tile.astype(jnp.bfloat16)
        outs[r * HALVES + HALVES - 1][128:136, :] = table.astype(jnp.bfloat16)


def rows_of(h):
    return 128 + 8 * (h == HALVES - 1)


def spectrum(waves, mask):
    shapes = [
        pltpu.VMEM((rows_of(h), 128), jnp.bfloat16)
        for _ in range(4)
        for h in range(HALVES)
    ]
    vmem = pl.BlockSpec(memory_space=pltpu.VMEM)
    return pl.pallas_call(
        spectrum_kernel,
        out_shape=shapes,
        in_specs=[pl.BlockSpec(memory_space=pltpu.SMEM)] + [vmem] * 3,
        out_specs=[vmem] * len(shapes),
        scratch_shapes=[
            pltpu.VMEM((4, 512, 256), jnp.float32),
            pltpu.VMEM((512, 256), jnp.float32),
            pltpu.VMEM((2, 512, 128), jnp.float32),
            pltpu.VMEM((64, 128), jnp.float32),
        ],
        compiler_params=pltpu.CompilerParams(vmem_limit_bytes=24 << 20),
        name="spectrum",
    )(mask, waves, jnp.asarray(twiddles()), jnp.asarray(second_dft()))


def correlate_kernel(h, decay_ref, *refs):
    last = h == HALVES - 1
    refs = list(refs)
    take = lambda n: [refs.pop(0) for _ in range(n)]
    pairs, planes = take(4), take(8)
    (table_hbm,) = take(1)
    before = take(1)[0] if h else None
    outs = take(2) if last else take(1)
    held, own, cross, total, inverse, table, spot, sem = take(8)
    z, mate = spots()
    fetch = pltpu.make_async_copy(table_hbm.at[2 * mate + h], table, sem)
    fetch.start()
    for r in range(4):
        for k in range(PB):
            p = pairs[r][0, k]
            dz = ((p // 4) - z + 8) % 8
            spot[(mate ^ r) * PB + k] = 4 * dz + ((p % 4) ^ mate)
    for r in range(4):
        own[r] = planes[0][r].astype(jnp.float32)
    for dz in range(8):
        for r in range(4):
            held[4 * dz + r] = planes[dz][r]

    def per_pair(step, carry):
        q, k = step // PB, step % PB
        theirs, mine = spot[step], q ^ mate
        tiles = [held[theirs, 16 * e : 16 * e + 16, :].astype(jnp.float32) for e in range(SEGS)]
        if last:
            marks = held[theirs, 128:136, :].astype(jnp.float32)
        for i in range(LS):
            real, imag = None, None
            for e in range(SEGS):
                pr, pi = tiles[e][:8], tiles[e][8:]
                at = 16 * e + i
                mr = jnp.broadcast_to(own[mine, at : at + 1, :], (8, 128))
                mi = jnp.broadcast_to(own[mine, at + 8 : at + 9, :], (8, 128))
                real = add(real, mr * pr)
                real = add(real, mi * pi)
                imag = add(imag, mr * pi)
                imag = sub(imag, mi * pr)
            at = pl.ds(pl.multiple_of(i * 128 + q * 32 + k * 8, 8), 8)
            cross[at, :128] = real
            cross[at, 128:] = imag
            if last:
                inverse[at, :] = own[mine, 128 + i : 129 + i, :] * marks
        return carry

    lax.fori_loop(0, 4 * PB, per_pair, 0)
    if last:
        ones = jnp.ones((128, 128), jnp.bfloat16)
        count = jnp.dot(
            inverse[...].astype(jnp.bfloat16), ones, preferred_element_type=jnp.float32
        )
        inverse[...] = 1.0 / jnp.maximum(count, 1.0)
    fetch.wait()
    lagged = total if last else outs[0]

    def per_rows(step, carry):
        at = pl.ds(pl.multiple_of(step * 256, 256), 256)
        spectra = cross[at, :].astype(jnp.bfloat16)
        part = jnp.dot(spectra, table[...], preferred_element_type=jnp.float32)
        lagged[at, :] = part + before[at, :] if h else part
        return carry

    lax.fori_loop(0, 4, per_rows, 0)
    if not last:
        return
    decay = jnp.full((8, 128), decay_ref[0], jnp.float32)
    high = decay.astype(jnp.bfloat16)
    low = (decay - high.astype(jnp.float32)).astype(jnp.bfloat16)
    both = jnp.where(row_of(8) < 4, high.astype(jnp.float32), low.astype(jnp.float32))

    core = mate % 2

    def per_part(n, carry):
        i, y = n // 2, n % 2
        for keep in range(2):
            q = 2 * y + (core ^ keep)
            at = pl.ds(pl.multiple_of(i * 128 + q * 32, 32), 32)
            part = inverse[at, :]
            for g in range(3):
                value = total[at, 128 * g : 128 * (g + 1)] * part
                outs[keep][n, 32 * g : 32 * (g + 1), :] = value.astype(jnp.bfloat16)
            marks = jnp.zeros_like(both) if keep else both
            outs[keep][n, 96:104, :] = marks.astype(jnp.bfloat16)
        return carry

    lax.fori_loop(0, 16, per_part, 0)


def row_of(n):
    return lax.broadcasted_iota(jnp.int32, (n, 128), 0)


def held_in_vmem(arrays):
    return [pltpu.with_memory_space_constraint(a, pltpu.VMEM) for a in arrays]


def correlate(h, decay, pairs, planes, table, carried):
    last = h == HALVES - 1
    smem, vmem = pl.BlockSpec(memory_space=pltpu.SMEM), pl.BlockSpec(memory_space=pltpu.VMEM)
    if last:
        shapes = [pltpu.VMEM((16, 104, 128), jnp.bfloat16)] * 2
    else:
        shapes = [pltpu.VMEM((1024, LAGS), jnp.float32)]
    return pl.pallas_call(
        functools.partial(correlate_kernel, h),
        out_shape=shapes,
        in_specs=[smem] * 5
        + [vmem] * 8
        + [pl.BlockSpec(memory_space=pl.ANY)]
        + [vmem] * len(carried),
        out_specs=[vmem] * len(shapes),
        scratch_shapes=[
            pltpu.VMEM((32, rows_of(h), 128), jnp.bfloat16),
            pltpu.VMEM((4, rows_of(h), 128), jnp.float32),
            pltpu.VMEM((1024, 256), jnp.float32),
            pltpu.VMEM((1024 if last else 8, LAGS), jnp.float32),
            pltpu.VMEM((1024 if last else 8, 128), jnp.float32),
            pltpu.VMEM((256, LAGS), jnp.bfloat16),
            pltpu.SMEM((4 * PB,), jnp.int32),
            pltpu.SemaphoreType.DMA,
        ],
        compiler_params=pltpu.CompilerParams(vmem_limit_bytes=24 << 20),
    )(
        decay,
        *pairs,
        *held_in_vmem(planes),
        pltpu.with_memory_space_constraint(table, pltpu.HBM),
        *held_in_vmem(carried),
    )


def scan_kernel(parts, out):
    state = [jnp.zeros((32, 128), jnp.float32)] * 3
    for w in range(8):
        marks = parts[2 * w, 96:104, :].astype(jnp.float32)
        decay = marks[:1] + marks[4:5]
        for g in range(3):
            at = slice(32 * g, 32 * (g + 1))
            lagged = parts[2 * w, at, :].astype(jnp.float32)
            lagged = lagged + parts[2 * w + 1, at, :].astype(jnp.float32)
            state[g] = decay * state[g] + lagged
            out[w, :, 128 * g : 128 * (g + 1)] = state[g].astype(jnp.bfloat16)


def scan_windows(parts):
    vmem = pl.BlockSpec(memory_space=pltpu.VMEM)
    return pl.pallas_call(
        scan_kernel,
        out_shape=jax.ShapeDtypeStruct((8, 32, LAGS), jnp.bfloat16),
        in_specs=[vmem],
        out_specs=vmem,
        compiler_params=pltpu.CompilerParams(vmem_limit_bytes=24 << 20),
        name="scan",
    )(parts)


def across(value, r):
    return lax.ppermute(value, ("y", "c"), [(d, d ^ r) for d in range(4)])


def along(value, step):
    return lax.ppermute(value, "z", [(d, (d + step) % 8) for d in range(8)])


def body(waveforms, segment_mask, pair_blocks, window_decay):
    pair_blocks = jnp.maximum(pair_blocks, 0)
    pairs = [pair_blocks] + [across(pair_blocks, r) for r in (1, 2, 3)]
    flat = spectrum(waveforms[0], segment_mask)
    table = jnp.asarray(lag_table())
    carried = []
    for h in range(HALVES):
        mine = [flat[r * HALVES + h] for r in range(4)]
        plane = jnp.stack([mine[0]] + [across(mine[r], r) for r in (1, 2, 3)])
        planes = [plane] + [None] * 7
        ahead = back = plane
        for step in range(1, 5):
            if step < 4 or h % 2 == 0:
                ahead = along(ahead, 1)
                planes[8 - step] = ahead
            if step < 4 or h % 2 == 1:
                back = along(back, -1)
                planes[step] = back
        carried = correlate(h, window_decay, pairs, planes, table, carried)
    kept, sent = carried
    kept = kept.astype(jnp.float32) + across(sent, 1).astype(jnp.float32)
    parts = lax.all_to_all(kept.astype(jnp.bfloat16), ("section", "y"), 0, 0)
    states = lax.all_to_all(scan_windows(parts), "section", 0, 0)
    return states[None]


def solution(mesh):
    split = Mesh(mesh.devices.reshape(8, 8, 2, 2), ("section", "z", "y", "c"))
    sta = ("z", "y", "c")
    placed = (P("section", sta, None, None), P("section", sta, None), P(sta, None), P("section"))

    return jax.shard_map(
        body,
        mesh=split,
        in_specs=placed,
        out_specs=P("section", sta, None, None),
        check_vma=False,
    )
```

```python
import functools
import math

import jax
import jax.numpy as jnp
import numpy as np
from jax import lax
from jax.experimental import pallas as pl
from jax.experimental.pallas import tpu as pltpu
from jax.sharding import Mesh
from jax.sharding import PartitionSpec as P


NF = 1024
LAGS = 384
NSAMP = 4096
LS = 8
SEGS = 8
PB = 4
EPSILON = 1e-05
HALVES = 2


def twiddles():
    k = np.arange(32)[:, None]
    b = np.arange(128)[None, :]
    angle = 2.0 * np.pi * (k * b) / NSAMP
    return np.stack([np.cos(angle), np.sin(angle)]).astype(np.float32)


def second_dft():
    b = np.arange(128)[:, None]
    m = np.arange(4, 36)[None, :]
    angle = 2.0 * np.pi * ((b * m) % 128) / 128
    cos, sin = np.cos(angle) / 64, np.sin(angle) / 64
    full = np.zeros((256, 256))
    full[:128, :32] = cos
    full[128:, :32] = sin
    full[:128, 128:160] = -sin
    full[128:, 128:160] = cos
    high = full.astype(jnp.bfloat16)
    low = (full - high.astype(np.float64)).astype(jnp.bfloat16)
    return np.stack([high, low])


def lag_table():
    freq = 128 + np.arange(NF)
    shift = np.arange(LAGS) + NSAMP - LAGS // 2
    phase = (freq[:, None] * shift[None, :] % NSAMP).astype(np.float32)
    phase = phase * np.float32(2.0 * np.pi / NSAMP)
    cos = np.cos(phase) / np.float32(math.sqrt(NF))
    sin = -np.sin(phase) / np.float32(math.sqrt(NF))
    lane = np.arange(128)
    rows = []
    for c in range(8):
        f = 8 * (lane // 32) + c + 32 * (lane % 32)
        rows += [cos[f], sin[f]]
    return np.concatenate(rows).reshape(8, 256, LAGS).astype(jnp.bfloat16)


def add(a, b):
    return b if a is None else a if b is None else a + b


def sub(a, b):
    if b is None:
        return a
    return -b if a is None else a - b


def real_fft(xs):
    n = len(xs)
    if n == 1:
        return [(xs[0], None)]
    if n == 2:
        return [(xs[0] + xs[1], None), (xs[0] - xs[1], None)]
    even, odd = real_fft(xs[0::2]), real_fft(xs[1::2])
    out = [None] * (n // 2 + 1)
    for k in range(n // 4 + 1):
        (er, ei), (orr, oi) = even[k], odd[k]
        if k == 0:
            tr, ti = orr, oi
        elif 4 * k == n:
            tr, ti = oi, None if orr is None else -orr
        else:
            c, s = math.cos(2 * math.pi * k / n), math.sin(2 * math.pi * k / n)
            if oi is None:
                tr, ti = orr * c, orr * (-s)
            else:
                tr, ti = orr * c + oi * s, oi * c - orr * s
        out[k] = (add(er, tr), add(ei, ti))
        out[n // 2 - k] = (sub(er, tr), sub(ti, ei))
    return out


def spots():
    core = lax.axis_index("c")
    return lax.axis_index("z"), 2 * lax.axis_index("y") + core, core


def spectrum_kernel(mask_hbm, pair_hbm, wave_hbm, turn_hbm, dft_hbm, *refs):
    outs, (mid, bins, white, marks) = refs[:-11], refs[-11:-7]
    mask_ref, pair_ref, wave_ref, turn_ref, dft_ref, wave_sem, sem = refs[-7:]
    turn_copy = pltpu.make_async_copy(turn_hbm, turn_ref, sem.at[0])
    late = [
        pltpu.make_async_copy(mask_hbm, mask_ref, sem.at[1]),
        pltpu.make_async_copy(pair_hbm, pair_ref, sem.at[2]),
        pltpu.make_async_copy(dft_hbm, dft_ref, sem.at[3]),
    ]

    def wave_copy(i):
        return pltpu.make_async_copy(wave_hbm.at[i], wave_ref.at[i], wave_sem.at[i])

    turn_copy.start()
    for i in range(LS):
        wave_copy(i).start()
    for copy in late:
        copy.start()
    turn_copy.wait()
    lane_at = lax.broadcasted_iota(jnp.int32, (LS, 128), 1)
    row_at = lax.broadcasted_iota(jnp.int32, (LS, 128), 0)

    def station(i, carry):
        wave_copy(i).wait()
        xs = [wave_ref[i, :, 128 * a : 128 * (a + 1)].astype(jnp.float32) for a in range(32)]
        half = real_fft(xs)
        for k in range(32):
            re, im = half[k] if k <= 16 else half[32 - k]
            if k > 16 and im is not None:
                im = -im
            if k:
                cos, sin = turn_ref[0, k : k + 1, :], turn_ref[1, k : k + 1, :]
                if im is None:
                    re, im = re * cos, -(re * sin)
                else:
                    re, im = re * cos + im * sin, im * cos - re * sin
            klo, c = divmod(k, 8)
            rows = pl.ds(pl.multiple_of(c * 64 + i * 8, 8), 8)
            mid[klo, rows, :128] = re
            mid[klo, rows, 128:] = jnp.zeros_like(re) if im is None else im
        return carry

    lax.fori_loop(0, LS, station, 0)
    for copy in late:
        copy.wait()

    def masks(i, table):
        mark = jnp.zeros((SEGS, 128), jnp.float32)
        for e in range(SEGS):
            valid = mask_ref[0, i, e].astype(jnp.float32)
            mark = jnp.where(row_at == e, valid, mark)
            table = jnp.where((row_at == i) & (lane_at == e), valid, table)
        marks[pl.ds(pl.multiple_of(i * 8, 8), 8), :] = mark
        return table

    table = lax.fori_loop(0, LS, masks, jnp.zeros((LS, 128), jnp.float32))
    for k in range(PB):
        table = jnp.where(lane_at == SEGS + k, pair_ref[0, k].astype(jnp.float32), table)
    dot = functools.partial(jnp.dot, preferred_element_type=jnp.float32)
    bins[...] = jnp.zeros_like(bins)

    def second(klo, carry):
        weights = []
        for part in range(2):
            base = dft_ref[part].astype(jnp.float32)
            sides = [pltpu.roll(base[:, at : at + 128], 32 * klo, 1) for at in (0, 128)]
            weights.append(jnp.concatenate(sides, axis=1).astype(jnp.bfloat16))
        wh, wl = weights
        value = mid[klo]
        high = value.astype(jnp.bfloat16)
        low = (value - high.astype(jnp.float32)).astype(jnp.bfloat16)
        bins[...] += dot(high, wh) + (dot(low, wh) + dot(high, wl))
        return carry

    lax.fori_loop(0, 4, second, 0)
    re, im = bins[:, :128], bins[:, 128:]
    amp = jnp.sqrt(re * re + im * im)
    amps = [amp[64 * c : 64 * (c + 1)] for c in range(8)]
    before, after = [amps[0]], [amps[7]]
    for c in range(1, 8):
        before.append(before[-1] + amps[c])
        after.append(after[-1] + amps[7 - c])
    after = after[::-1]
    total = before[7]
    lane = lax.broadcasted_iota(jnp.int32, (64, 128), 1)
    klo = lane // 32
    m = lane % 32
    turned = [pltpu.roll(total, 32 * d, 1) for d in (1, 2, 3)]
    zero = jnp.zeros_like(total)
    all_klo = total + turned[0] + turned[1] + turned[2]
    lower = upper = zero
    for d in (1, 2, 3):
        lower = lower + jnp.where(klo >= d, turned[d - 1], zero)
        upper = upper + jnp.where(klo + d <= 3, turned[3 - d], zero)
    for c in range(8):
        left = pltpu.roll(after[c] + upper, 1, 1)
        right = pltpu.roll(before[c] + lower, 127, 1)
        smooth = all_klo + jnp.where(m >= 1, left, zero) + jnp.where(m <= 30, right, zero)
        scale = marks[...] / (smooth * (1.0 / 65) + EPSILON)
        rows = slice(64 * c, 64 * (c + 1))
        white[0, rows, :] = re[rows] * scale
        white[1, rows, :] = im[rows] * scale
    _, mate, _ = spots()
    for r in range(4):
        for h in range(HALVES):
            out = outs[r * HALVES + h]
            first = 64 * (2 * (mate ^ r) + h)
            for seg in range(SEGS):
                at = pl.ds(first + seg, 8, stride=8)
                tile = jnp.concatenate([white[0, at, :], white[1, at, :]], axis=0)
                out[16 * seg : 16 * seg + 16, :] = tile.astype(jnp.bfloat16)
        outs[r * HALVES + HALVES - 1][128:136, :] = table.astype(jnp.bfloat16)


def rows_of(h):
    return 128 + 8 * (h == HALVES - 1)


def spectrum(waves, mask, pairs):
    shapes = [
        pltpu.VMEM((rows_of(h), 128), jnp.bfloat16)
        for _ in range(4)
        for h in range(HALVES)
    ]
    vmem = pl.BlockSpec(memory_space=pltpu.VMEM)
    args = [mask, pairs, waves, jnp.asarray(twiddles()), jnp.asarray(second_dft())]
    return pl.pallas_call(
        spectrum_kernel,
        out_shape=shapes,
        in_specs=[pl.BlockSpec(memory_space=pl.ANY)] * 5,
        out_specs=[vmem] * len(shapes),
        scratch_shapes=[
            pltpu.VMEM((4, 512, 256), jnp.float32),
            pltpu.VMEM((512, 256), jnp.float32),
            pltpu.VMEM((2, 512, 128), jnp.float32),
            pltpu.VMEM((64, 128), jnp.float32),
            pltpu.SMEM((1, LS, SEGS), jnp.int32),
            pltpu.SMEM((1, PB), jnp.int32),
            pltpu.VMEM((LS, SEGS, NSAMP), jnp.bfloat16),
            pltpu.VMEM((2, 32, 128), jnp.float32),
            pltpu.VMEM((2, 256, 256), jnp.bfloat16),
            pltpu.SemaphoreType.DMA((LS,)),
            pltpu.SemaphoreType.DMA((4,)),
        ],
        compiler_params=pltpu.CompilerParams(vmem_limit_bytes=24 << 20),
        name="spectrum",
    )(*[pltpu.with_memory_space_constraint(a, pltpu.HBM) for a in args])


def correlate_kernel(h, side, decay_ref, pair_ref, *refs):
    last = h == HALVES - 1
    refs = list(refs)
    take = lambda n: [refs.pop(0) for _ in range(n)]
    planes = take(8)
    (table_hbm,) = take(1)
    before = take(1)[0] if last else None
    (out,) = take(1)
    held, own, cross, total, inverse, table, spot, sem = take(8)
    z, mate, core = spots()
    sides = 1 if last else 2
    fetch = pltpu.make_async_copy(table_hbm.at[2 * mate + h], table, sem)
    fetch.start()
    for r in range(4):
        q = mate ^ r
        for k in range(PB):
            p = pair_ref[r, k]
            dz = ((p // 4) - z + 8) % 8
            spot[q * PB + k] = 4 * dz + ((p % 4) ^ mate)
    for r in range(4):
        own[r] = planes[0][r].astype(jnp.float32)
    for dz in range(8):
        for r in range(4):
            held[4 * dz + r] = planes[dz][r]

    def per_pair(step, carry):
        part, y, k = (side if last else step // 8), (step // PB) % 2, step % PB
        q = 2 * y + (core ^ part)
        theirs, mine = spot[q * PB + k], q ^ mate
        tiles = [held[theirs, 16 * e : 16 * e + 16, :].astype(jnp.float32) for e in range(SEGS)]
        if last:
            marks = held[theirs, 128:136, :].astype(jnp.float32)
        for i in range(LS):
            real, imag = None, None
            for e in range(SEGS):
                pr, pi = tiles[e][:8], tiles[e][8:]
                at = 16 * e + i
                mr = jnp.broadcast_to(own[mine, at : at + 1, :], (8, 128))
                mi = jnp.broadcast_to(own[mine, at + 8 : at + 9, :], (8, 128))
                real = add(real, mr * pr)
                real = add(real, mi * pi)
                imag = add(imag, mr * pi)
                imag = sub(imag, mi * pr)
            at = (step // 8) * 512 + i * 64 + y * 32 + k * 8
            at = pl.ds(pl.multiple_of(at, 8), 8)
            cross[at, :128] = real
            cross[at, 128:] = imag
            if last:
                inverse[at, :] = own[mine, 128 + i : 129 + i, :] * marks
        return carry

    lax.fori_loop(0, 8 * sides, per_pair, 0)
    if last:
        ones = jnp.where(row_of(128) < SEGS, 1.0, 0.0).astype(jnp.bfloat16)
        valid = inverse[...].astype(jnp.bfloat16)
        count = jnp.dot(valid, ones, preferred_element_type=jnp.float32)
        inverse[...] = 1.0 / jnp.maximum(count, 1.0)
    fetch.wait()
    lagged = total if last else out

    def per_rows(step, carry):
        at = pl.ds(pl.multiple_of(step * 256, 256), 256)
        spectra = cross[at, :].astype(jnp.bfloat16)
        part = jnp.dot(spectra, table[...], preferred_element_type=jnp.float32)
        if last:
            part = part + before[pl.ds(pl.multiple_of(side * 512 + step * 256, 256), 256), :]
        lagged[at, :] = part
        return carry

    lax.fori_loop(0, 2 * sides, per_rows, 0)
    if not last:
        return
    decay = jnp.full((8, 128), decay_ref[0], jnp.float32)
    high = decay.astype(jnp.bfloat16).astype(jnp.float32)
    both = jnp.where(row_of(8) < 4, high, decay - high)
    if side:
        both = jnp.zeros_like(both)

    def per_part(n, carry):
        at = pl.ds(pl.multiple_of(n * 32, 32), 32)
        part = inverse[at, :]
        for g in range(3):
            value = total[at, 128 * g : 128 * (g + 1)] * part
            out[n, 32 * g : 32 * (g + 1), :] = value.astype(jnp.bfloat16)
        out[n, 96:104, :] = both.astype(jnp.bfloat16)
        return carry

    lax.fori_loop(0, 16, per_part, 0)


def row_of(n):
    return lax.broadcasted_iota(jnp.int32, (n, 128), 0)


def held_in_vmem(arrays):
    return [pltpu.with_memory_space_constraint(a, pltpu.VMEM) for a in arrays]


def correlate(h, side, decay, pairs, planes, table, carried):
    last = h == HALVES - 1
    smem, vmem = pl.BlockSpec(memory_space=pltpu.SMEM), pl.BlockSpec(memory_space=pltpu.VMEM)
    rows = 512 if last else 1024
    if last:
        shape = pltpu.VMEM((16, 104, 128), jnp.bfloat16)
    else:
        shape = pltpu.VMEM((1024, LAGS), jnp.float32)
    return pl.pallas_call(
        functools.partial(correlate_kernel, h, side),
        out_shape=shape,
        in_specs=[smem] * 2
        + [vmem] * 8
        + [pl.BlockSpec(memory_space=pl.ANY)]
        + [vmem] * len(carried),
        out_specs=vmem,
        scratch_shapes=[
            pltpu.VMEM((32, rows_of(h), 128), jnp.bfloat16),
            pltpu.VMEM((4, rows_of(h), 128), jnp.float32),
            pltpu.VMEM((rows, 256), jnp.float32),
            pltpu.VMEM((rows if last else 8, LAGS), jnp.float32),
            pltpu.VMEM((rows if last else 8, 128), jnp.float32),
            pltpu.VMEM((256, LAGS), jnp.bfloat16),
            pltpu.SMEM((4 * PB,), jnp.int32),
            pltpu.SemaphoreType.DMA,
        ],
        compiler_params=pltpu.CompilerParams(vmem_limit_bytes=24 << 20),
    )(
        decay,
        pairs,
        *held_in_vmem(planes),
        pltpu.with_memory_space_constraint(table, pltpu.HBM),
        *held_in_vmem(carried),
    )


def scan_kernel(parts, out):
    state = [jnp.zeros((32, 128), jnp.float32)] * 3
    for w in range(8):
        marks = parts[2 * w, 96:104, :].astype(jnp.float32)
        decay = marks[:1] + marks[4:5]
        for g in range(3):
            at = slice(32 * g, 32 * (g + 1))
            lagged = parts[2 * w, at, :].astype(jnp.float32)
            lagged = lagged + parts[2 * w + 1, at, :].astype(jnp.float32)
            state[g] = decay * state[g] + lagged
            out[w, :, 128 * g : 128 * (g + 1)] = state[g].astype(jnp.bfloat16)


def scan_windows(parts):
    vmem = pl.BlockSpec(memory_space=pltpu.VMEM)
    return pl.pallas_call(
        scan_kernel,
        out_shape=jax.ShapeDtypeStruct((8, 32, LAGS), jnp.bfloat16),
        in_specs=[vmem],
        out_specs=vmem,
        compiler_params=pltpu.CompilerParams(vmem_limit_bytes=24 << 20),
        name="scan",
    )(parts)


def across(value, r):
    return lax.ppermute(value, ("y", "c"), [(d, d ^ r) for d in range(4)])


def along(value, step):
    return lax.ppermute(value, "z", [(d, (d + step) % 8) for d in range(8)])


def body(waveforms, segment_mask, pair_blocks, window_decay):
    flat = spectrum(waveforms[0], segment_mask, pair_blocks)
    table = jnp.asarray(lag_table())
    halves = []
    for h in range(HALVES):
        mine = [flat[r * HALVES + h] for r in range(4)]
        plane = jnp.stack([mine[0]] + [across(mine[r], r) for r in (1, 2, 3)])
        planes = [plane] + [None] * 7
        ahead = back = plane
        for step in range(1, 5):
            if step < 4 or h % 2 == 0:
                ahead = along(ahead, 1)
                planes[8 - step] = ahead
            if step < 4 or h % 2 == 1:
                back = along(back, -1)
                planes[step] = back
        halves.append(planes)
    pairs = halves[1][0][:, 128, SEGS : SEGS + PB].astype(jnp.int32)
    lagged = correlate(0, 0, window_decay, pairs, halves[0], table, [])
    sent = correlate(1, 1, window_decay, pairs, halves[1], table, [lagged])
    kept = correlate(1, 0, window_decay, pairs, halves[1], table, [lagged])
    kept = kept.astype(jnp.float32) + across(sent, 1).astype(jnp.float32)
    parts = lax.all_to_all(kept.astype(jnp.bfloat16), ("section", "y"), 0, 0)
    states = lax.all_to_all(scan_windows(parts), "section", 0, 0)
    return states[None]


def solution(mesh):
    split = Mesh(mesh.devices.reshape(8, 8, 2, 2), ("section", "z", "y", "c"))
    sta = ("z", "y", "c")
    placed = (P("section", sta, None, None), P("section", sta, None), P(sta, None), P("section"))

    return jax.shard_map(
        body,
        mesh=split,
        in_specs=placed,
        out_specs=P("section", sta, None, None),
        check_vma=False,
    )
```

```python
import functools
import math

import jax
import jax.numpy as jnp
import numpy as np
from jax import lax
from jax.experimental import pallas as pl
from jax.experimental.pallas import tpu as pltpu
from jax.sharding import Mesh
from jax.sharding import PartitionSpec as P


NF = 1024
LAGS = 384
NSAMP = 4096
LS = 8
SEGS = 8
PB = 4
EPSILON = 1e-05
HALVES = 2


def twiddles():
    k = np.arange(32)[:, None]
    b = np.arange(128)[None, :]
    angle = 2.0 * np.pi * (k * b) / NSAMP
    return np.stack([np.cos(angle), np.sin(angle)]).astype(np.float32)


def second_dft():
    b = np.arange(128)[:, None]
    m = np.arange(4, 36)[None, :]
    angle = 2.0 * np.pi * ((b * m) % 128) / 128
    cos, sin = np.cos(angle) / 64, np.sin(angle) / 64
    full = np.zeros((256, 256))
    full[:128, :32] = cos
    full[128:, :32] = sin
    full[:128, 128:160] = -sin
    full[128:, 128:160] = cos
    high = full.astype(jnp.bfloat16)
    low = (full - high.astype(np.float64)).astype(jnp.bfloat16)
    return np.stack([high, low])


def lag_table():
    freq = 128 + np.arange(NF)
    shift = np.arange(LAGS) + NSAMP - LAGS // 2
    phase = (freq[:, None] * shift[None, :] % NSAMP).astype(np.float32)
    phase = phase * np.float32(2.0 * np.pi / NSAMP)
    cos = np.cos(phase) / np.float32(math.sqrt(NF))
    sin = -np.sin(phase) / np.float32(math.sqrt(NF))
    lane = np.arange(128)
    rows = []
    for c in range(8):
        f = 8 * (lane // 32) + c + 32 * (lane % 32)
        rows += [cos[f], sin[f]]
    return np.concatenate(rows).reshape(8, 256, LAGS).astype(jnp.bfloat16)


def add(a, b):
    return b if a is None else a if b is None else a + b


def sub(a, b):
    if b is None:
        return a
    return -b if a is None else a - b


def real_fft(xs):
    n = len(xs)
    if n == 1:
        return [(xs[0], None)]
    if n == 2:
        return [(xs[0] + xs[1], None), (xs[0] - xs[1], None)]
    even, odd = real_fft(xs[0::2]), real_fft(xs[1::2])
    out = [None] * (n // 2 + 1)
    for k in range(n // 4 + 1):
        (er, ei), (orr, oi) = even[k], odd[k]
        if k == 0:
            tr, ti = orr, oi
        elif 4 * k == n:
            tr, ti = oi, None if orr is None else -orr
        else:
            c, s = math.cos(2 * math.pi * k / n), math.sin(2 * math.pi * k / n)
            if oi is None:
                tr, ti = orr * c, orr * (-s)
            else:
                tr, ti = orr * c + oi * s, oi * c - orr * s
        out[k] = (add(er, tr), add(ei, ti))
        out[n // 2 - k] = (sub(er, tr), sub(ti, ei))
    return out


def spots():
    core = lax.axis_index("c")
    return lax.axis_index("z"), 2 * lax.axis_index("y") + core, core


def spectrum_kernel(mask_hbm, pair_hbm, wave_hbm, turn_hbm, dft_hbm, *refs):
    outs, (mid, bins, white, marks) = refs[:-11], refs[-11:-7]
    mask_ref, pair_ref, wave_ref, turn_ref, dft_ref, wave_sem, sem = refs[-7:]
    turn_copy = pltpu.make_async_copy(turn_hbm, turn_ref, sem.at[0])
    late = [
        pltpu.make_async_copy(mask_hbm, mask_ref, sem.at[1]),
        pltpu.make_async_copy(pair_hbm, pair_ref, sem.at[2]),
        pltpu.make_async_copy(dft_hbm, dft_ref, sem.at[3]),
    ]

    def wave_copy(i):
        return pltpu.make_async_copy(wave_hbm.at[i], wave_ref.at[i], wave_sem.at[i])

    turn_copy.start()
    for i in range(LS):
        wave_copy(i).start()
    for copy in late:
        copy.start()
    turn_copy.wait()
    lane_at = lax.broadcasted_iota(jnp.int32, (LS, 128), 1)
    row_at = lax.broadcasted_iota(jnp.int32, (LS, 128), 0)

    def station(i, carry):
        wave_copy(i).wait()
        xs = [wave_ref[i, :, 128 * a : 128 * (a + 1)].astype(jnp.float32) for a in range(32)]
        half = real_fft(xs)
        for k in range(32):
            re, im = half[k] if k <= 16 else half[32 - k]
            if k > 16 and im is not None:
                im = -im
            if k:
                cos, sin = turn_ref[0, k : k + 1, :], turn_ref[1, k : k + 1, :]
                if im is None:
                    re, im = re * cos, -(re * sin)
                else:
                    re, im = re * cos + im * sin, im * cos - re * sin
            klo, c = divmod(k, 8)
            rows = pl.ds(pl.multiple_of(c * 64 + i * 8, 8), 8)
            mid[klo, rows, :128] = re
            mid[klo, rows, 128:] = jnp.zeros_like(re) if im is None else im
        return carry

    lax.fori_loop(0, LS, station, 0)
    for copy in late:
        copy.wait()

    def masks(i, table):
        mark = jnp.zeros((SEGS, 128), jnp.float32)
        for e in range(SEGS):
            valid = mask_ref[0, i, e].astype(jnp.float32)
            mark = jnp.where(row_at == e, valid, mark)
            table = jnp.where((row_at == i) & (lane_at == e), valid, table)
        marks[pl.ds(pl.multiple_of(i * 8, 8), 8), :] = mark
        return table

    table = lax.fori_loop(0, LS, masks, jnp.zeros((LS, 128), jnp.float32))
    for k in range(PB):
        table = jnp.where(lane_at == SEGS + k, pair_ref[0, k].astype(jnp.float32), table)
    dot = functools.partial(jnp.dot, preferred_element_type=jnp.float32)
    bins[...] = jnp.zeros_like(bins)

    def second(klo, carry):
        weights = []
        for part in range(2):
            base = dft_ref[part].astype(jnp.float32)
            sides = [pltpu.roll(base[:, at : at + 128], 32 * klo, 1) for at in (0, 128)]
            weights.append(jnp.concatenate(sides, axis=1).astype(jnp.bfloat16))
        wh, wl = weights
        value = mid[klo]
        high = value.astype(jnp.bfloat16)
        low = (value - high.astype(jnp.float32)).astype(jnp.bfloat16)
        bins[...] += dot(high, wh) + (dot(low, wh) + dot(high, wl))
        return carry

    lax.fori_loop(0, 4, second, 0)
    re, im = bins[:, :128], bins[:, 128:]
    amp = jnp.sqrt(re * re + im * im)
    amps = [amp[64 * c : 64 * (c + 1)] for c in range(8)]
    before, after = [amps[0]], [amps[7]]
    for c in range(1, 8):
        before.append(before[-1] + amps[c])
        after.append(after[-1] + amps[7 - c])
    after = after[::-1]
    total = before[7]
    lane = lax.broadcasted_iota(jnp.int32, (64, 128), 1)
    klo = lane // 32
    m = lane % 32
    turned = [pltpu.roll(total, 32 * d, 1) for d in (1, 2, 3)]
    zero = jnp.zeros_like(total)
    all_klo = total + turned[0] + turned[1] + turned[2]
    lower = upper = zero
    for d in (1, 2, 3):
        lower = lower + jnp.where(klo >= d, turned[d - 1], zero)
        upper = upper + jnp.where(klo + d <= 3, turned[3 - d], zero)
    for c in range(8):
        left = pltpu.roll(after[c] + upper, 1, 1)
        right = pltpu.roll(before[c] + lower, 127, 1)
        smooth = all_klo + jnp.where(m >= 1, left, zero) + jnp.where(m <= 30, right, zero)
        scale = marks[...] / (smooth * (1.0 / 65) + EPSILON)
        rows = slice(64 * c, 64 * (c + 1))
        white[0, rows, :] = re[rows] * scale
        white[1, rows, :] = im[rows] * scale
    _, mate, _ = spots()
    for r in range(4):
        for h in range(HALVES):
            out = outs[r * HALVES + h]
            first = 64 * (2 * (mate ^ r) + h)
            for seg in range(SEGS):
                at = pl.ds(first + seg, 8, stride=8)
                tile = jnp.concatenate([white[0, at, :], white[1, at, :]], axis=0)
                out[16 * seg : 16 * seg + 16, :] = tile.astype(jnp.bfloat16)
        outs[r * HALVES + HALVES - 1][128:136, :] = table.astype(jnp.bfloat16)


def rows_of(h):
    return 128 + 8 * (h == HALVES - 1)


def spectrum(waves, mask, pairs):
    shapes = [
        pltpu.VMEM((rows_of(h), 128), jnp.bfloat16)
        for _ in range(4)
        for h in range(HALVES)
    ]
    vmem = pl.BlockSpec(memory_space=pltpu.VMEM)
    args = [mask, pairs, waves, jnp.asarray(twiddles()), jnp.asarray(second_dft())]
    return pl.pallas_call(
        spectrum_kernel,
        out_shape=shapes,
        in_specs=[pl.BlockSpec(memory_space=pl.ANY)] * 5,
        out_specs=[vmem] * len(shapes),
        scratch_shapes=[
            pltpu.VMEM((4, 512, 256), jnp.float32),
            pltpu.VMEM((512, 256), jnp.float32),
            pltpu.VMEM((2, 512, 128), jnp.float32),
            pltpu.VMEM((64, 128), jnp.float32),
            pltpu.SMEM((1, LS, SEGS), jnp.int32),
            pltpu.SMEM((1, PB), jnp.int32),
            pltpu.VMEM((LS, SEGS, NSAMP), jnp.bfloat16),
            pltpu.VMEM((2, 32, 128), jnp.float32),
            pltpu.VMEM((2, 256, 256), jnp.bfloat16),
            pltpu.SemaphoreType.DMA((LS,)),
            pltpu.SemaphoreType.DMA((4,)),
        ],
        compiler_params=pltpu.CompilerParams(vmem_limit_bytes=24 << 20),
        name="spectrum",
    )(*[pltpu.with_memory_space_constraint(a, pltpu.HBM) for a in args])


def correlate_kernel(h, side, decay_ref, pair_ref, *refs):
    last = h == HALVES - 1
    refs = list(refs)
    take = lambda n: [refs.pop(0) for _ in range(n)]
    planes = take(8)
    (table_hbm,) = take(1)
    before = take(1)[0] if last else None
    (out,) = take(1)
    held, own, cross, total, inverse, table, spot, sem = take(8)
    z, mate, core = spots()
    sides = 1 if last else 2
    fetch = pltpu.make_async_copy(table_hbm.at[2 * mate + h], table, sem)
    fetch.start()
    for r in range(4):
        q = mate ^ r
        for k in range(PB):
            p = pair_ref[r, k]
            dz = ((p // 4) - z + 8) % 8
            spot[q * PB + k] = 4 * dz + ((p % 4) ^ mate)
    for r in range(4):
        own[r] = planes[0][r].astype(jnp.float32)
    for dz in range(8):
        for r in range(4):
            held[4 * dz + r] = planes[dz][r]

    def per_pair(step, carry):
        part, y, k = (side if last else step // 8), (step // PB) % 2, step % PB
        q = 2 * y + (core ^ part)
        theirs, mine = spot[q * PB + k], q ^ mate
        tiles = [held[theirs, 16 * e : 16 * e + 16, :].astype(jnp.float32) for e in range(SEGS)]
        if last:
            marks = held[theirs, 128:136, :].astype(jnp.float32)
        for i in range(LS):
            real, imag = None, None
            for e in range(SEGS):
                pr, pi = tiles[e][:8], tiles[e][8:]
                at = 16 * e + i
                mr = jnp.broadcast_to(own[mine, at : at + 1, :], (8, 128))
                mi = jnp.broadcast_to(own[mine, at + 8 : at + 9, :], (8, 128))
                real = add(real, mr * pr)
                real = add(real, mi * pi)
                imag = add(imag, mr * pi)
                imag = sub(imag, mi * pr)
            at = (step // 8) * 512 + i * 64 + y * 32 + k * 8
            at = pl.ds(pl.multiple_of(at, 8), 8)
            cross[at, :128] = real
            cross[at, 128:] = imag
            if last:
                inverse[at, :] = own[mine, 128 + i : 129 + i, :] * marks
        return carry

    lax.fori_loop(0, 8 * sides, per_pair, 0)
    if last:
        ones = jnp.where(row_of(128) < SEGS, 1.0, 0.0).astype(jnp.bfloat16)
        valid = inverse[...].astype(jnp.bfloat16)
        count = jnp.dot(valid, ones, preferred_element_type=jnp.float32)
        inverse[...] = 1.0 / jnp.maximum(count, 1.0)
    fetch.wait()
    lagged = total if last else out

    def per_rows(step, carry):
        at = pl.ds(pl.multiple_of(step * 256, 256), 256)
        spectra = cross[at, :].astype(jnp.bfloat16)
        part = jnp.dot(spectra, table[...], preferred_element_type=jnp.float32)
        if last:
            part = part + before[pl.ds(pl.multiple_of(side * 512 + step * 256, 256), 256), :]
        lagged[at, :] = part
        return carry

    lax.fori_loop(0, 2 * sides, per_rows, 0)
    if not last:
        return
    decay = jnp.full((8, 128), decay_ref[0], jnp.float32)
    high = decay.astype(jnp.bfloat16).astype(jnp.float32)
    both = jnp.where(row_of(8) < 4, high, decay - high)
    if side:
        both = jnp.zeros_like(both)

    def per_part(step, carry):
        at = pl.ds(pl.multiple_of(step * 32, 32), 32)
        i, y = step // 2, step % 2
        n = (i // 2) * 4 + y * 2 + i % 2
        part = inverse[at, :]
        for g in range(3):
            value = total[at, 128 * g : 128 * (g + 1)] * part
            out[n, 32 * g : 32 * (g + 1), :] = value.astype(jnp.bfloat16)
        out[n, 96:104, :] = both.astype(jnp.bfloat16)
        return carry

    lax.fori_loop(0, 16, per_part, 0)


def row_of(n):
    return lax.broadcasted_iota(jnp.int32, (n, 128), 0)


def held_in_vmem(arrays):
    return [pltpu.with_memory_space_constraint(a, pltpu.VMEM) for a in arrays]


def correlate(h, side, decay, pairs, planes, table, carried):
    last = h == HALVES - 1
    smem, vmem = pl.BlockSpec(memory_space=pltpu.SMEM), pl.BlockSpec(memory_space=pltpu.VMEM)
    rows = 512 if last else 1024
    if last:
        shape = pltpu.VMEM((16, 104, 128), jnp.bfloat16)
    else:
        shape = pltpu.VMEM((1024, LAGS), jnp.float32)
    return pl.pallas_call(
        functools.partial(correlate_kernel, h, side),
        out_shape=shape,
        in_specs=[smem] * 2
        + [vmem] * 8
        + [pl.BlockSpec(memory_space=pl.ANY)]
        + [vmem] * len(carried),
        out_specs=vmem,
        scratch_shapes=[
            pltpu.VMEM((32, rows_of(h), 128), jnp.bfloat16),
            pltpu.VMEM((4, rows_of(h), 128), jnp.float32),
            pltpu.VMEM((rows, 256), jnp.float32),
            pltpu.VMEM((rows if last else 8, LAGS), jnp.float32),
            pltpu.VMEM((rows if last else 8, 128), jnp.float32),
            pltpu.VMEM((256, LAGS), jnp.bfloat16),
            pltpu.SMEM((4 * PB,), jnp.int32),
            pltpu.SemaphoreType.DMA,
        ],
        compiler_params=pltpu.CompilerParams(vmem_limit_bytes=24 << 20),
    )(
        decay,
        pairs,
        *held_in_vmem(planes),
        pltpu.with_memory_space_constraint(table, pltpu.HBM),
        *held_in_vmem(carried),
    )


def scan_kernel(rescan, parts, *refs):
    x = lax.axis_index("x")
    for e in range(2):
        for g in range(3):
            at = slice(32 * g, 32 * (g + 1))
            if rescan:
                state = refs[0][e, at, :].astype(jnp.float32)
            else:
                state = jnp.zeros((32, 128), jnp.float32)
            for w in range(4):
                marks = parts[2 * w, 0, 96:104, :].astype(jnp.float32)
                decay = marks[:1] + marks[4:5]
                lagged = parts[2 * w, e, at, :].astype(jnp.float32)
                lagged = lagged + parts[2 * w + 1, e, at, :].astype(jnp.float32)
                state = decay * state + lagged
                if rescan:
                    value = state.astype(jnp.bfloat16)
                    refs[5][w, 32 * e : 32 * (e + 1), 128 * g : 128 * (g + 1)] = value
            if not rescan:
                refs[0][e, at, :] = state.astype(jnp.bfloat16)
    if rescan:
        for r in range(4):
            refs[1 + r][...] = refs[5][x ^ r]


def scan_windows(parts, entering):
    vmem = pl.BlockSpec(memory_space=pltpu.VMEM)
    if entering:
        shapes = [pltpu.VMEM((64, LAGS), jnp.bfloat16)] * 4
    else:
        shapes = [pltpu.VMEM((2, 96, 128), jnp.bfloat16)]
    return pl.pallas_call(
        functools.partial(scan_kernel, bool(entering)),
        out_shape=shapes,
        in_specs=[vmem] * (1 + len(entering)),
        out_specs=[vmem] * len(shapes),
        scratch_shapes=[pltpu.VMEM((4, 64, LAGS), jnp.bfloat16)] if entering else [],
        compiler_params=pltpu.CompilerParams(vmem_limit_bytes=24 << 20),
        name="rescan" if entering else "scan",
    )(*held_in_vmem([parts, *entering]))


def gather_kernel(*refs):
    ins, out, sem = refs[:4], refs[4], refs[5]
    x = lax.axis_index("x")
    copies = [pltpu.make_async_copy(ins[r], out.at[x ^ r], sem.at[r]) for r in range(4)]
    for copy in copies:
        copy.start()
    for copy in copies:
        copy.wait()


def gather_stations(ins):
    return pl.pallas_call(
        gather_kernel,
        out_shape=pltpu.HBM((4, 64, LAGS), jnp.bfloat16),
        in_specs=[pl.BlockSpec(memory_space=pltpu.VMEM)] * 4,
        out_specs=pl.BlockSpec(memory_space=pl.ANY),
        scratch_shapes=[pltpu.SemaphoreType.DMA((4,))],
        compiler_params=pltpu.CompilerParams(vmem_limit_bytes=24 << 20),
        name="gather",
    )(*held_in_vmem(ins))


def across(value, r):
    return lax.ppermute(value, ("y", "c"), [(d, d ^ r) for d in range(4)])


def along(value, step):
    return lax.ppermute(value, "z", [(d, (d + step) % 8) for d in range(8)])


def body(waveforms, segment_mask, pair_blocks, window_decay):
    flat = spectrum(waveforms[0], segment_mask, pair_blocks)
    table = jnp.asarray(lag_table())
    halves = []
    for h in range(HALVES):
        mine = [flat[r * HALVES + h] for r in range(4)]
        plane = jnp.stack([mine[0]] + [across(mine[r], r) for r in (1, 2, 3)])
        planes = [plane] + [None] * 7
        ahead = back = plane
        for step in range(1, 5):
            if step < 4 or h % 2 == 0:
                ahead = along(ahead, 1)
                planes[8 - step] = ahead
            if step < 4 or h % 2 == 1:
                back = along(back, -1)
                planes[step] = back
        halves.append(planes)
    pairs = halves[1][0][:, 128, SEGS : SEGS + PB].astype(jnp.int32)
    lagged = correlate(0, 0, window_decay, pairs, halves[0], table, [])
    sent = correlate(1, 1, window_decay, pairs, halves[1], table, [lagged])
    kept = correlate(1, 0, window_decay, pairs, halves[1], table, [lagged])
    kept = kept.astype(jnp.float32) + across(sent, 1).astype(jnp.float32)
    kept = kept.astype(jnp.bfloat16).reshape(8, 2, 104, 128)
    parts = lax.all_to_all(kept, ("x", "y"), 0, 0)
    (total,) = scan_windows(parts, [])
    entering = lax.ppermute(total, "yh", [(0, 1)])
    states = list(scan_windows(parts, [entering]))
    for r in (1, 2, 3):
        states[r] = lax.ppermute(states[r], "x", [(d, d ^ r) for d in range(4)])
    return gather_stations(states).reshape(1, LS, 32, LAGS)


def solution(mesh):
    split = Mesh(mesh.devices.reshape(2, 4, 8, 2, 2), ("yh", "x", "z", "y", "c"))
    sta = ("z", "y", "c")
    section = ("yh", "x")
    placed = (P(section, sta, None, None), P(section, sta, None), P(sta, None), P(section))

    return jax.shard_map(
        body,
        mesh=split,
        in_specs=placed,
        out_specs=P(section, sta, None, None),
        check_vma=False,
    )
```
